32 devices in a mesh: dp: 8 (over z, core), row: 2 (over x), col: 2 (over y).
Axes of the slice: x: 2, y: 2, z: 4, core: 2. Of those that a mesh axis runs over, the one named last changes fastest.
Arguments:
- tokens: bfloat16 [4096, 8192], P(('dp', 'row', 'col')), parts along dimension 0, may hold values from -6 to 6
- w_gate: bfloat16 [8192, 1024], P(('row', 'col')), may hold values from -0.0625 to 0.0625
- w_up: bfloat16 [8192, 1024], P(('row', 'col')), may hold values from -0.0625 to 0.0625
- w_down: bfloat16 [1024, 8192], P(None, ('row', 'col')), may hold values from -0.1875 to 0.1875
Outputs:
- mixed: bfloat16 [4096, 8192], P(('dp', 'row', 'col')), parts along dimension 0
The draws below stay inside these ranges and needn't reach their ends.
There are 8 independent parts, one for each index of `dp`. The reference program is written for one: setup_inputs(seed, part) draws one part's arguments, and reference() takes and returns one part's arrays. A program takes and returns all parts, laid end to end along the dimension named above; an argument that names none is the same for every part. Nothing has to cross between parts.
All inputs are finite; a program needn't handle non-finite values.
Results may differ from the reference program's by a relative error of at most 0.029.
Values may be sent and summed in bfloat16 or wider, within the bound.
A program may use at most 64 MiB of HBM per device.

```python
import jax
import jax.numpy as jnp
from jax import lax

D = 8192
H = 1024
TOKENS = 512
N_ROW = 2


def block_scale(rng, shape, pieces, low, largest):
    loudness = 1.0
    for axis_at, shards_of in pieces:
        draws = jax.random.uniform(jax.random.fold_in(jax.random.fold_in(rng, 6), axis_at), (shards_of,), jnp.float32, low / len(pieces), largest / len(pieces))
        loudness = loudness * jnp.repeat(jnp.exp(draws), shape[axis_at] // shards_of).reshape((-1,) + (1,) * (len(shape) - 1 - axis_at))
    return loudness


def noise(own_key, shape, width, bound, shards=(), dtype=jnp.bfloat16):
    level = block_scale(own_key, shape, shards, -0.22, 0.18) if shards else 1.0
    entries = jax.random.normal(own_key, shape, jnp.float32) * width * level
    return jnp.minimum(jnp.maximum(entries, -bound), bound).astype(dtype)


def setup_inputs(seed: int = 0, part: int = 0) -> dict:
    seeds = jax.random.split(jax.random.key(seed), 5)
    part_splits = jax.random.split(jax.random.fold_in(seeds[4], part), 5)
    return {
        "tokens": noise(part_splits[0], (TOKENS, D), 1.0, 6.0, ((0, 4),)),
        "w_gate": noise(seeds[1], (D, H), D ** -0.5, 0.0625, ((0, 4),)),
        "w_up": noise(seeds[2], (D, H), D ** -0.5, 0.0625, ((0, 4),)),
        "w_down": noise(seeds[3], (H, D), H ** -0.5, 0.1875, ((1, 4),)),
    }


def reference(tokens, w_gate, w_up, w_down):
    slab_width = D // N_ROW
    paired = jnp.concatenate([w_gate, w_up], axis=1)
    running = jnp.zeros((tokens.shape[0], 2 * H), jnp.float32)
    for block_index in range(N_ROW):
        lower = block_index * slab_width
        upper = lower + slab_width
        partial_value = jnp.dot(tokens[:, lower:upper], paired[lower:upper], preferred_element_type=jnp.float32)
        rounded = lax.optimization_barrier(partial_value.astype(jnp.bfloat16))
        running = running + rounded.astype(jnp.float32)
    hidden = (jax.nn.silu(running[:, :H]) * running[:, H:]).astype(jnp.bfloat16)
    return jnp.dot(hidden, w_down, preferred_element_type=jnp.float32).astype(jnp.bfloat16)
```

```python
import functools

import jax
import jax.numpy as jnp
from jax import lax
from jax.experimental import pallas as pl
from jax.experimental.pallas import tpu as pltpu
from jax.sharding import PartitionSpec as P

MESH = pl.DeviceIdType.MESH
CHUNKS = 4
EARLY_HOPS = 2
ORDER = (
    "fetch", "project 0", "project 1", "hop 1", "project 2", "project 3", "hop 2", "combine 0", "combine 1",
    "last hops", "combine 2", "activate 0", "combine 3", "activate 1", "activate 2", "activate 3",
    "emit 0", "emit 1", "local", "emit 2", "emit 3", "landed", "emit fetched",
)


def tile_of(width, most):
    tile = min(width, most)
    while width % tile:
        tile //= 2
    return tile


def kernel(
    groups, rows, cols, chunks,
    x_ref, wg_ref, wu_ref, wd_ref, out_ref,
    wg, wu, wa, wb, xbuf, acc, part, rec_a, rec_b, sum_a, sum_b, fin_a, fin_b, ha, hb, oa, ob,
    w_sem, fa_sem, fb_sem, up_sem, down_sem, land_sem, mate_sem,
    x_sem, a_sem, b_sem, c_sem, d_sem, ha_sem, hb_sem, oa_sem, ob_sem, ga_sem, gb_sem,
):
    n = rows * cols
    row, col = lax.axis_index("row"), lax.axis_index("col")
    group = lax.axis_index("dp")
    mates = 2 - groups % 2
    planes = groups // mates
    plane, core = group // mates, lax.rem(group, mates)
    t = x_ref.shape[0] // chunks
    features, hidden = wg.shape
    half = hidden // 2
    side_cols = wa.shape[2]
    share = hidden // groups
    bf16, f32 = jnp.bfloat16, jnp.float32

    def up(r, c):
        return lax.rem(row + r, rows), lax.rem(col + c, cols)

    def down(r, c):
        return lax.rem(row + rows - r, rows), lax.rem(col + cols - c, cols)

    def shard(rc, width):
        return pl.ds(pl.multiple_of((rc[0] * cols + rc[1]) * width, width), width)

    def remote(src, dst, sems, index, to):
        return pltpu.make_async_remote_copy(
            src_ref=src, dst_ref=dst,
            send_sem=sems.at[(0, *index)], recv_sem=sems.at[(1, *index)],
            device_id={"row": to[0], "col": to[1]}, device_id_type=MESH,
        )

    def tok(k):
        return pl.ds(pl.multiple_of(k * t, t), t)

    slots = [(r, c) for r in range(rows) for c in range(cols)]
    others = slots[1:]
    by_reach = others[::-1]

    def at_slot(r, c):
        return pl.ds((r * cols + c) * t, t)

    def x_copy(k, r, c):
        to = up(r, c)
        return remote(
            x_ref.at[tok(k), shard(to, features)], xbuf.at[k, at_slot(r, c)],
            x_sem, (k, r * cols + c), to,
        )

    def x_own(k):
        return pltpu.make_async_copy(
            x_ref.at[tok(k), shard((row, col), features)], xbuf.at[k, at_slot(0, 0)], x_sem.at[1, k, 0]
        )

    def a_copy(k, r):
        return remote(part.at[k, 0, r], rec_a.at[k, r], a_sem, (k, r), down(r, 0))

    def b_copy(k, c):
        return remote(part.at[k, 1, :, c], rec_b.at[k, c], b_sem, (k, c), down(0, c))

    def c_copy(k, c):
        return remote(sum_a.at[k, c], fin_a.at[k, c], c_sem, (k, c), down(0, c))

    def d_copy(k, r):
        return remote(sum_b.at[k, r], fin_b.at[k, r], d_sem, (k, r), down(r, 0))

    def share_of(g):
        return pl.ds(pl.multiple_of(g * share, share), share)

    def fetch_a(c):
        return remote(
            wd_ref.at[share_of(group), pl.ds(0, side_cols)], wa.at[c, share_of(group)],
            fa_sem, (c,), down(0, c),
        )

    def fetch_b(r):
        return remote(
            wd_ref.at[share_of(group), pl.ds(side_cols, side_cols)], wb.at[r, share_of(group)],
            fb_sem, (r,), down(r, 0),
        )

    blocks_a = [(wa, c, c) for c in range(1, cols)]
    blocks_b = [(wb, r, cols + r) for r in range(1, rows)]
    blocks = blocks_a + blocks_b

    def pass_on(source, block, sems, to_plane):
        ref, slot, index = block
        region = ref.at[slot, share_of(source * mates + core)]
        return pltpu.make_async_remote_copy(
            src_ref=region, dst_ref=region,
            send_sem=sems.at[source, index], recv_sem=land_sem.at[source, index],
            device_id={"dp": to_plane * mates + core}, device_id_type=MESH,
        )

    def to_mate(source, block, whose):
        ref, slot, index = block
        region = ref.at[slot, share_of(source * mates + whose)]
        return pltpu.make_async_remote_copy(
            src_ref=region, dst_ref=region,
            send_sem=mate_sem.at[0, source, index], recv_sem=mate_sem.at[1, source, index],
            device_id={"dp": plane * mates + (mates - 1 - core)}, device_id_type=MESH,
        )

    def spread(source, some, upward, downward):
        for block in some:
            if upward:

                @pl.when(plane + 1 < planes)
                def _():
                    pass_on(source, block, up_sem, plane + 1).start()

            if downward:

                @pl.when(plane > 0)
                def _():
                    pass_on(source, block, down_sem, plane - 1).start()

            if mates > 1:
                to_mate(source, block, core).start()

    def hop(h, some):
        below, above = plane - h, plane + h

        @pl.when(below >= 0)
        def _():
            for block in some:
                pass_on(below, block, up_sem, plane).wait_recv()
            spread(below, some, True, False)

        @pl.when(above < planes)
        def _():
            for block in some:
                pass_on(above, block, down_sem, plane).wait_recv()
            spread(above, some, False, True)

    def last_hops():
        def more(h, _):
            hop(h, blocks_a)
            hop(h, blocks_b)
            return 0

        lax.fori_loop(EARLY_HOPS + 1, planes, more, 0)

    def landed():
        if mates > 1:

            def from_mate(z, _):
                for block in blocks:
                    to_mate(z, block, mates - 1 - core).wait_recv()
                return 0

            lax.fori_loop(0, planes, from_mate, 0)

    def sent(z, _):
        for block in blocks:
            if mates > 1:
                to_mate(z, block, core).wait_send()

            @pl.when(jnp.logical_and(plane + 1 < planes, z <= plane))
            def _():
                pass_on(z, block, up_sem, plane).wait_send()

            @pl.when(jnp.logical_and(plane > 0, z >= plane))
            def _():
                pass_on(z, block, down_sem, plane).wait_send()

        return 0

    def ha_copy(k, r):
        return remote(ha.at[0, tok(k)], ha.at[r, tok(k)], ha_sem, (k, r), up(r, 0))

    def hb_copy(k, c):
        return remote(hb.at[0, tok(k)], hb.at[c, tok(k)], hb_sem, (k, c), up(0, c))

    def columns(rc, side, start, width):
        base = (rc[0] * cols + rc[1]) * 2 * side_cols + side * side_cols + start
        return pl.ds(pl.multiple_of(base, width), width)

    def oa_copy(k, r, columns_of):
        return remote(
            oa.at[0, r - 1, tok(k)], out_ref.at[tok(k), columns(columns_of, 0, 0, side_cols)],
            oa_sem, (k, r), down(r, 0),
        )

    def ob_copy(k, c, columns_of):
        return remote(
            ob.at[0, c - 1, tok(k)], out_ref.at[tok(k), columns(columns_of, 1, 0, side_cols)],
            ob_sem, (k, c), down(0, c),
        )

    out_tile = tile_of(side_cols, 256)
    out_tiles = side_cols // out_tile

    def ga_copy(c, j, r, columns_of):
        return remote(
            oa.at[c, r - 1, :, pl.ds(j * out_tile, out_tile)],
            out_ref.at[:, columns(columns_of, 0, j * out_tile, out_tile)],
            ga_sem, (c, j, r), down(r, 0),
        )

    def gb_copy(r, j, c, columns_of):
        return remote(
            ob.at[r, c - 1, :, pl.ds(j * out_tile, out_tile)],
            out_ref.at[:, columns(columns_of, 1, j * out_tile, out_tile)],
            gb_sem, (r, j, c), down(0, c),
        )

    loads = [
        pltpu.make_async_copy(wg_ref, wg, w_sem.at[0]),
        pltpu.make_async_copy(wu_ref, wu, w_sem.at[1]),
        pltpu.make_async_copy(wd_ref.at[:, pl.ds(0, side_cols)], wa.at[0], w_sem.at[2]),
        pltpu.make_async_copy(wd_ref.at[:, pl.ds(side_cols, side_cols)], wb.at[0], w_sem.at[3]),
    ]

    barrier = pltpu.get_barrier_semaphore()
    for r, c in others:
        to = up(r, c)
        pl.semaphore_signal(barrier, inc=1, device_id={"row": to[0], "col": to[1]}, device_id_type=MESH)

    def greet(g):
        pl.semaphore_signal(barrier, inc=1, device_id={"dp": g}, device_id_type=MESH)

    pl.when(plane > 0)(lambda: greet(group - mates))
    pl.when(plane + 1 < planes)(lambda: greet(group + mates))
    if mates > 1:
        greet(plane * mates + (mates - 1 - core))
    neighbours = (plane > 0).astype(jnp.int32) + (plane + 1 < planes).astype(jnp.int32)
    for k in range(chunks):
        x_own(k).start()
    for load in loads:
        load.start()
    pl.semaphore_wait(barrier, n - 1 + mates - 1 + neighbours)

    for c in range(1, cols):
        fetch_a(c).start()
    for r in range(1, rows):
        fetch_b(r).start()
    for k in range(chunks):
        for r, c in by_reach:
            x_copy(k, r, c).start()

    def fetch():
        for c in range(1, cols):
            fetch_a(c).wait_recv()
        spread(plane, blocks_a, True, True)
        for r in range(1, rows):
            fetch_b(r).wait_recv()
        spread(plane, blocks_b, True, True)
        for load in loads:
            load.wait()

    tile = tile_of(half, 512)
    per_half = half // tile

    def project(k):
        x_own(k).wait()
        for r, c in others:
            x_copy(k, r, c).wait_recv()

        def column(j, _):
            side, at = j // per_half, lax.rem(j, per_half) * tile
            source = pl.ds(pl.multiple_of(j * tile, tile), tile)
            for w, base in ((wg, 0), (wu, half)):
                target = pl.ds(pl.multiple_of(base + at, tile), tile)
                got = jnp.dot(xbuf[k], w[:, source], preferred_element_type=f32)
                acc[k, side, :, target] = got[:t]
                for r, c in others:
                    first = (r * cols + c) * t
                    part[k, side, r, c, :, target] = got[first : first + t].astype(bf16)
            return 0

        lax.fori_loop(0, 2 * per_half, column, 0)
        for r in range(1, rows):
            a_copy(k, r).start()
        for c in range(1, cols):
            b_copy(k, c).start()

    def combine(k):
        for r in range(1, rows):
            a_copy(k, r).wait_recv()
        for c in range(1, cols):
            total = part[k, 0, 0, c].astype(f32)
            for r in range(1, rows):
                total = total + rec_a[k, r, c].astype(f32)
            sum_a[k, c] = total.astype(bf16)
            c_copy(k, c).start()
        for c in range(1, cols):
            b_copy(k, c).wait_recv()
        for r in range(1, rows):
            total = part[k, 1, r, 0].astype(f32)
            for c in range(1, cols):
                total = total + rec_b[k, c, r].astype(f32)
            sum_b[k, r] = total.astype(bf16)
            d_copy(k, r).start()

    def activate(k):
        for c in range(1, cols):
            c_copy(k, c).wait_recv()
        for r in range(1, rows):
            d_copy(k, r).wait_recv()
        for side in range(2):
            total = acc[k, side]
            if side == 0:
                for r in range(1, rows):
                    total = total + rec_a[k, r, 0].astype(f32)
                for c in range(1, cols):
                    total = total + fin_a[k, c].astype(f32)
            else:
                for c in range(1, cols):
                    total = total + rec_b[k, c, 0].astype(f32)
                for r in range(1, rows):
                    total = total + fin_b[k, r].astype(f32)
            gate = total[:, :half]
            done = (gate / (1.0 + jnp.exp(-gate)) * total[:, half:]).astype(bf16)
            ha[0, tok(k), pl.ds(side * half, half)] = done
            hb[0, tok(k), pl.ds(side * half, half)] = done
        for r in range(1, rows):
            ha_copy(k, r).start()
        for c in range(1, cols):
            hb_copy(k, c).start()

    wide = tile_of(side_cols, 512)
    wides = side_cols // wide

    def emit(k):
        for r in range(1, rows):
            ha_copy(k, r).wait_recv()
        theirs = ha[pl.ds(1, rows - 1), tok(k)].reshape((rows - 1) * t, hidden)
        for j in range(wides):
            where = pl.ds(j * wide, wide)
            got = jnp.dot(theirs, wa[0, :, where], preferred_element_type=f32).astype(bf16)
            oa[0, :, tok(k), where] = got.reshape(rows - 1, t, wide)
        for r in range(1, rows):
            oa_copy(k, r, (row, col)).start()
        for c in range(1, cols):
            hb_copy(k, c).wait_recv()
        theirs = hb[pl.ds(1, cols - 1), tok(k)].reshape((cols - 1) * t, hidden)
        for j in range(wides):
            where = pl.ds(j * wide, wide)
            got = jnp.dot(theirs, wb[0, :, where], preferred_element_type=f32).astype(bf16)
            ob[0, :, tok(k), where] = got.reshape(cols - 1, t, wide)
        for c in range(1, cols):
            ob_copy(k, c, (row, col)).start()

    def local():
        def columns_of(j, _):
            where = pl.ds(pl.multiple_of(j * wide, wide), wide)
            for side, w in ((0, wa), (1, wb)):
                out_ref[:, columns((row, col), side, j * wide, wide)] = jnp.dot(
                    ha[0], w[0, :, where], preferred_element_type=f32
                ).astype(bf16)
            return 0

        lax.fori_loop(0, wides, columns_of, 0)

    count = t * chunks

    def fetched_a(i):
        c, j = 1 + i // out_tiles, lax.rem(i, out_tiles)
        where = pl.ds(pl.multiple_of(j * out_tile, out_tile), out_tile)
        got = jnp.dot(
            ha[...].reshape(rows * count, hidden), wa[c, :, where], preferred_element_type=f32
        ).astype(bf16)
        oa[c, :, :, where] = got[count:].reshape(rows - 1, count, out_tile)
        for r in range(1, rows):
            ga_copy(c, j, r, up(0, c)).start()
        out_ref[:, columns(up(0, c), 0, j * out_tile, out_tile)] = got[:count]

    def fetched_b(i):
        r, j = 1 + i // out_tiles, lax.rem(i, out_tiles)
        where = pl.ds(pl.multiple_of(j * out_tile, out_tile), out_tile)
        got = jnp.dot(
            hb[...].reshape(cols * count, hidden), wb[r, :, where], preferred_element_type=f32
        ).astype(bf16)
        ob[r, :, :, where] = got[count:].reshape(cols - 1, count, out_tile)
        for c in range(1, cols):
            gb_copy(r, j, c, up(r, 0)).start()
        out_ref[:, columns(up(r, 0), 1, j * out_tile, out_tile)] = got[:count]

    tiles_a, tiles_b = (cols - 1) * out_tiles, (rows - 1) * out_tiles
    both = min(tiles_a, tiles_b)

    def emit_fetched():
        def pair(i, _):
            fetched_a(i)
            fetched_b(i)
            return 0

        def only(one):
            def body(i, _):
                one(i)
                return 0

            return body

        lax.fori_loop(0, both, pair, 0)
        lax.fori_loop(both, tiles_a, only(fetched_a), 0)
        lax.fori_loop(both, tiles_b, only(fetched_b), 0)

    def both_hops(h):
        hop(h, blocks_a)
        hop(h, blocks_b)

    stages = {"project": project, "combine": combine, "activate": activate, "emit": emit}
    once = {
        "fetch": fetch, "last hops": last_hops, "landed": landed, "local": local, "emit fetched": emit_fetched,
    }
    for task in ORDER:
        if task in once:
            once[task]()
        else:
            name, at = task.split()
            if name == "hop":
                if int(at) < planes:
                    both_hops(int(at))
            else:
                stages[name](int(at))

    def finish(k, _):
        for r, c in others:
            x_copy(k, r, c).wait_send()
        for r in range(1, rows):
            oa_copy(k, r, (row, col)).wait_send()
            oa_copy(k, r, up(r, 0)).wait_recv()
            a_copy(k, r).wait_send()
            d_copy(k, r).wait_send()
            ha_copy(k, r).wait_send()
        for c in range(1, cols):
            ob_copy(k, c, (row, col)).wait_send()
            ob_copy(k, c, up(0, c)).wait_recv()
            b_copy(k, c).wait_send()
            c_copy(k, c).wait_send()
            hb_copy(k, c).wait_send()
        return 0

    lax.fori_loop(0, chunks, finish, 0)

    def finish_fetched(j, _):
        for c in range(1, cols):
            for r in range(1, rows):
                ga_copy(c, j, r, up(0, c)).wait_send()
                ga_copy(c, j, r, up(r, c)).wait_recv()
                gb_copy(r, j, c, up(r, 0)).wait_send()
                gb_copy(r, j, c, up(r, c)).wait_recv()
        return 0

    lax.fori_loop(0, out_tiles, finish_fetched, 0)
    for c in range(1, cols):
        fetch_a(c).wait_send()
    for r in range(1, rows):
        fetch_b(r).wait_send()
    lax.fori_loop(0, planes, sent, 0)


def solution(mesh):
    groups, rows, cols = mesh.shape["dp"], mesh.shape["row"], mesh.shape["col"]
    planes = groups // (2 - groups % 2)
    n = rows * cols

    def shards(tokens, w_gate, w_up, w_down):
        count, width = tokens.shape
        features, hidden = w_gate.shape
        side_cols = w_down.shape[1] // 2
        chunks = CHUNKS
        t = count // chunks
        out_tiles = side_cols // tile_of(side_cols, 256)
        bf16 = jnp.bfloat16
        any_space = pl.BlockSpec(memory_space=pl.ANY)

        def sems(*shape):
            return pltpu.SemaphoreType.DMA((2, chunks, *shape))

        return pl.pallas_call(
            functools.partial(kernel, groups, rows, cols, chunks),
            out_shape=pltpu.VMEM((count, width), bf16),
            in_specs=[any_space] * 4,
            out_specs=pl.BlockSpec(memory_space=pltpu.VMEM),
            scratch_shapes=[
                pltpu.VMEM((features, hidden), bf16),
                pltpu.VMEM((features, hidden), bf16),
                pltpu.VMEM((cols, hidden, side_cols), bf16),
                pltpu.VMEM((rows, hidden, side_cols), bf16),
                pltpu.VMEM((chunks, n * t, features), bf16),
                pltpu.VMEM((chunks, 2, t, hidden), jnp.float32),
                pltpu.VMEM((chunks, 2, rows, cols, t, hidden), bf16),
                pltpu.VMEM((chunks, rows, cols, t, hidden), bf16),
                pltpu.VMEM((chunks, cols, rows, t, hidden), bf16),
                pltpu.VMEM((chunks, cols, t, hidden), bf16),
                pltpu.VMEM((chunks, rows, t, hidden), bf16),
                pltpu.VMEM((chunks, cols, t, hidden), bf16),
                pltpu.VMEM((chunks, rows, t, hidden), bf16),
                pltpu.VMEM((rows, count, hidden), bf16),
                pltpu.VMEM((cols, count, hidden), bf16),
                pltpu.VMEM((cols, rows - 1, count, side_cols), bf16),
                pltpu.VMEM((rows, cols - 1, count, side_cols), bf16),
                pltpu.SemaphoreType.DMA((4,)),
                pltpu.SemaphoreType.DMA((2, cols)),
                pltpu.SemaphoreType.DMA((2, rows)),
                pltpu.SemaphoreType.DMA((planes, cols + rows)),
                pltpu.SemaphoreType.DMA((planes, cols + rows)),
                pltpu.SemaphoreType.DMA((planes, cols + rows)),
                pltpu.SemaphoreType.DMA((2, planes, cols + rows)),
                sems(n), sems(rows), sems(cols), sems(cols), sems(rows),
                sems(rows), sems(cols), sems(rows), sems(cols),
                pltpu.SemaphoreType.DMA((2, cols, out_tiles, rows)),
                pltpu.SemaphoreType.DMA((2, rows, out_tiles, cols)),
            ],
            compiler_params=pltpu.CompilerParams(collective_id=0, has_side_effects=True),
        )(tokens, w_gate, w_up, w_down)

    in_specs = (
        P(("dp", "row", "col"), None),
        P(("row", "col"), None),
        P(("row", "col"), None),
        P(None, ("row", "col")),
    )
    out_specs = P(("dp", "row", "col"), None)
    return jax.shard_map(shards, mesh=mesh, in_specs=in_specs, out_specs=out_specs, check_vma=False)
```

```python
import functools

import jax
import jax.numpy as jnp
from jax import lax
from jax.experimental import pallas as pl
from jax.experimental.pallas import tpu as pltpu
from jax.sharding import PartitionSpec as P

MESH = pl.DeviceIdType.MESH
CHUNKS = 4
EARLY_HOPS = 2
ORDER = (
    "fetch", "project 0", "project 1", "hop 1", "project 2", "project 3", "hop 2", "combine 0", "combine 1",
    "combine 2", "combine 3", "activate 0", "activate 1", "activate 2", "activate 3", "emit 0", "emit 1",
    "last hops", "local", "emit 2", "emit 3", "landed", "emit fetched",
)
X, A, B, C, D, HA, HB, OA, OB, FA, FB, ZA, ZB, MA, MB = range(15)


def tile_of(width, most):
    tile = min(width, most)
    while width % tile:
        tile //= 2
    return tile


def kernel(
    groups, rows, cols, chunks,
    x_ref, wg_ref, wu_ref, wd_ref, out_ref,
    xin, wf, wg, wu, wa, wb, xbuf, acc, part, rec_a, rec_b, sum_a, sum_b, fin_a, fin_b, ha, hb, oa, ob,
    load_sem, sent_sem, x_sem, step_sem, fetch_sem, land_sem, mate_sem, out_sem,
):
    n = rows * cols
    row, col = lax.axis_index("row"), lax.axis_index("col")
    group = lax.axis_index("dp")
    mates = 2
    planes = groups // mates
    plane, core = group // mates, lax.rem(group, mates)
    count = x_ref.shape[0]
    t = count // chunks
    features, hidden = wg.shape
    half = hidden // 2
    side_cols = wa.shape[2]
    share = hidden // groups
    bf16, f32 = jnp.bfloat16, jnp.float32

    def up(r, c):
        return lax.rem(row + r, rows), lax.rem(col + c, cols)

    def down(r, c):
        return lax.rem(row + rows - r, rows), lax.rem(col + cols - c, cols)

    def shard(rc, width):
        return pl.ds(pl.multiple_of((rc[0] * cols + rc[1]) * width, width), width)

    def remote(src, dst, kind, landing, to):
        return pltpu.make_async_remote_copy(
            src_ref=src, dst_ref=dst, send_sem=sent_sem.at[kind], recv_sem=landing,
            device_id={"row": to[0], "col": to[1]}, device_id_type=MESH,
        )

    def all_sent(kind, ref):
        remote(ref, ref, kind, out_sem.at[0], up(rows - 1, cols - 1)).wait_send()

    def all_here(landing, ref):
        remote(ref, ref, 0, landing, up(rows - 1, cols - 1)).wait_recv()

    def tok(k):
        return pl.ds(k * t, t)

    others = [(r, c) for r in range(rows) for c in range(cols)][1:]
    by_reach = others[::-1]
    rest_rows, rest_cols = pl.ds(1, rows - 1), pl.ds(1, cols - 1)

    def x_copy(k, r, c):
        to = up(r, c)
        return remote(
            xin.at[tok(k), shard(to, features)], xbuf.at[k, pl.ds((r * cols + c) * t, t)], X, x_sem.at[k], to
        )

    def a_copy(k, r):
        return remote(part.at[k, 0, r], rec_a.at[k, r], A, step_sem.at[0, k], down(r, 0))

    def b_copy(k, c):
        return remote(part.at[k, 1, :, c], rec_b.at[k, c], B, step_sem.at[1, k], down(0, c))

    def c_copy(k, c):
        return remote(sum_a.at[k, c], fin_a.at[k, c], C, step_sem.at[2, k], down(0, c))

    def d_copy(k, r):
        return remote(sum_b.at[k, r], fin_b.at[k, r], D, step_sem.at[3, k], down(r, 0))

    def ha_copy(k, r):
        return remote(ha.at[0, tok(k)], ha.at[r, tok(k)], HA, step_sem.at[4, k], up(r, 0))

    def hb_copy(k, c):
        return remote(hb.at[0, tok(k)], hb.at[c, tok(k)], HB, step_sem.at[5, k], up(0, c))

    def share_of(g):
        return pl.ds(pl.multiple_of(g * share, share), share)

    def fetch_a(c):
        return remote(wf.at[0], wa.at[c, share_of(group)], FA, fetch_sem.at[0], down(0, c))

    def fetch_b(r):
        return remote(wf.at[1], wb.at[r, share_of(group)], FB, fetch_sem.at[1], down(r, 0))

    sides = ((wa, rest_cols), (wb, rest_rows))

    def pass_on(source, side, to_plane):
        ref, rest = sides[side]
        region = ref.at[rest, share_of(source * mates + core)]
        return pltpu.make_async_remote_copy(
            src_ref=region, dst_ref=region, send_sem=sent_sem.at[ZA + side], recv_sem=land_sem.at[source, side],
            device_id={"dp": to_plane * mates + core}, device_id_type=MESH,
        )

    def to_mate(source, side):
        ref, rest = sides[side]
        region = ref.at[rest, share_of(source * mates + core)]
        return pltpu.make_async_remote_copy(
            src_ref=region, dst_ref=region, send_sem=sent_sem.at[MA + side], recv_sem=mate_sem.at[side],
            device_id={"dp": plane * mates + (mates - 1 - core)}, device_id_type=MESH,
        )

    def spread(source, side, upward, downward):
        if upward:
            pl.when(plane + 1 < planes)(lambda: pass_on(source, side, plane + 1).start())
        if downward:
            pl.when(plane > 0)(lambda: pass_on(source, side, plane - 1).start())
        to_mate(source, side).start()

    def hop(h):
        below, above = plane - h, plane + h
        for side in range(2):

            @pl.when(below >= 0)
            def _():
                pass_on(below, side, plane).wait_recv()
                spread(below, side, True, False)

            @pl.when(above < planes)
            def _():
                pass_on(above, side, plane).wait_recv()
                spread(above, side, False, True)

    def last_hops():
        def more(h, _):
            hop(h)
            return 0

        lax.fori_loop(EARLY_HOPS + 1, planes, more, 0)

    def landed():
        for side, (ref, rest) in enumerate(sides):
            all_here(mate_sem.at[side], ref.at[rest, pl.ds(0, planes * share)])

    def columns(rc, side, start, width):
        base = (rc[0] * cols + rc[1]) * 2 * side_cols + side * side_cols + start
        return pl.ds(pl.multiple_of(base, width), width)

    def oa_copy(k, r):
        return remote(
            oa.at[0, r - 1, tok(k)], out_ref.at[tok(k), columns((row, col), 0, 0, side_cols)],
            OA, out_sem.at[0], down(r, 0),
        )

    def ob_copy(k, c):
        return remote(
            ob.at[0, c - 1, tok(k)], out_ref.at[tok(k), columns((row, col), 1, 0, side_cols)],
            OB, out_sem.at[1], down(0, c),
        )

    out_tile = tile_of(side_cols, 256)
    out_tiles = side_cols // out_tile

    def ga_copy(c, j, r):
        return remote(
            oa.at[c, r - 1, :, pl.ds(pl.multiple_of(j * out_tile, out_tile), out_tile)],
            out_ref.at[:, columns(up(0, c), 0, j * out_tile, out_tile)],
            OA, out_sem.at[0], down(r, 0),
        )

    def gb_copy(r, j, c):
        return remote(
            ob.at[r, c - 1, :, pl.ds(pl.multiple_of(j * out_tile, out_tile), out_tile)],
            out_ref.at[:, columns(up(r, 0), 1, j * out_tile, out_tile)],
            OB, out_sem.at[1], down(0, c),
        )

    own_share = share_of(group)
    first_loads = [
        pltpu.make_async_copy(wd_ref.at[own_share, pl.ds(0, side_cols)], wf.at[0], load_sem.at[0]),
        pltpu.make_async_copy(wd_ref.at[own_share, pl.ds(side_cols, side_cols)], wf.at[1], load_sem.at[1]),
        pltpu.make_async_copy(x_ref, xin, load_sem.at[2]),
    ]
    own = [
        pltpu.make_async_copy(
            x_ref.at[tok(k), shard((row, col), features)], xbuf.at[k, pl.ds(0, t)], load_sem.at[3 + k]
        )
        for k in range(chunks)
    ]
    loads = [
        pltpu.make_async_copy(wg_ref, wg, load_sem.at[3 + chunks]),
        pltpu.make_async_copy(wu_ref, wu, load_sem.at[4 + chunks]),
        pltpu.make_async_copy(wd_ref.at[:, pl.ds(0, side_cols)], wa.at[0], load_sem.at[5 + chunks]),
        pltpu.make_async_copy(wd_ref.at[:, pl.ds(side_cols, side_cols)], wb.at[0], load_sem.at[6 + chunks]),
    ]

    barrier = pltpu.get_barrier_semaphore()
    for r, c in others:
        to = up(r, c)
        pl.semaphore_signal(barrier, inc=1, device_id={"row": to[0], "col": to[1]}, device_id_type=MESH)

    def greet(g):
        pl.semaphore_signal(barrier, inc=1, device_id={"dp": g}, device_id_type=MESH)

    pl.when(plane > 0)(lambda: greet(group - mates))
    pl.when(plane + 1 < planes)(lambda: greet(group + mates))
    greet(plane * mates + (mates - 1 - core))
    neighbours = (plane > 0).astype(jnp.int32) + (plane + 1 < planes).astype(jnp.int32)
    for load in first_loads:
        load.start()
    for load in first_loads:
        load.wait()
    pl.semaphore_wait(barrier, n - 1 + mates - 1 + neighbours)

    for c in range(1, cols):
        fetch_a(c).start()
    for r in range(1, rows):
        fetch_b(r).start()
    for k in range(chunks):
        for r, c in by_reach:
            x_copy(k, r, c).start()
    for load in own + loads:
        load.start()

    def fetch():
        all_here(fetch_sem.at[0], wa.at[rest_cols, own_share])
        spread(plane, 0, True, True)
        all_here(fetch_sem.at[1], wb.at[rest_rows, own_share])
        spread(plane, 1, True, True)
        for load in loads:
            load.wait()

    tile = tile_of(half, 512)
    per_half = half // tile

    def project(k):
        own[k].wait()
        all_here(x_sem.at[k], xbuf.at[k, pl.ds(t, (n - 1) * t)])

        def column(j, _):
            side, at = j // per_half, lax.rem(j, per_half) * tile
            source = pl.ds(pl.multiple_of(j * tile, tile), tile)
            for w, base in ((wg, 0), (wu, half)):
                target = pl.ds(pl.multiple_of(base + at, tile), tile)
                got = jnp.dot(xbuf[k], w[:, source], preferred_element_type=f32)
                acc[k, side, :, target] = got[:t]
                for r, c in others:
                    first = (r * cols + c) * t
                    part[k, side, r, c, :, target] = got[first : first + t].astype(bf16)
            return 0

        lax.fori_loop(0, 2 * per_half, column, 0)
        for r in range(1, rows):
            a_copy(k, r).start()
        for c in range(1, cols):
            b_copy(k, c).start()

    def combine(k):
        all_here(step_sem.at[0, k], rec_a.at[k, rest_rows])
        for c in range(1, cols):
            total = part[k, 0, 0, c].astype(f32)
            for r in range(1, rows):
                total = total + rec_a[k, r, c].astype(f32)
            sum_a[k, c] = total.astype(bf16)
            c_copy(k, c).start()
        all_here(step_sem.at[1, k], rec_b.at[k, rest_cols])
        for r in range(1, rows):
            total = part[k, 1, r, 0].astype(f32)
            for c in range(1, cols):
                total = total + rec_b[k, c, r].astype(f32)
            sum_b[k, r] = total.astype(bf16)
            d_copy(k, r).start()

    def activate(k):
        all_here(step_sem.at[2, k], fin_a.at[k, rest_cols])
        all_here(step_sem.at[3, k], fin_b.at[k, rest_rows])
        for side in range(2):
            total = acc[k, side]
            if side == 0:
                for r in range(1, rows):
                    total = total + rec_a[k, r, 0].astype(f32)
                for c in range(1, cols):
                    total = total + fin_a[k, c].astype(f32)
            else:
                for c in range(1, cols):
                    total = total + rec_b[k, c, 0].astype(f32)
                for r in range(1, rows):
                    total = total + fin_b[k, r].astype(f32)
            gate = total[:, :half]
            done = (gate / (1.0 + jnp.exp(-gate)) * total[:, half:]).astype(bf16)
            ha[0, tok(k), pl.ds(side * half, half)] = done
            hb[0, tok(k), pl.ds(side * half, half)] = done
        for r in range(1, rows):
            ha_copy(k, r).start()
        for c in range(1, cols):
            hb_copy(k, c).start()

    wide = tile_of(side_cols, 512)
    wides = side_cols // wide

    def emit(k):
        all_here(step_sem.at[4, k], ha.at[rest_rows, tok(k)])
        theirs = ha[rest_rows, tok(k)].reshape((rows - 1) * t, hidden)
        for j in range(wides):
            where = pl.ds(j * wide, wide)
            got = jnp.dot(theirs, wa[0, :, where], preferred_element_type=f32).astype(bf16)
            oa[0, :, tok(k), where] = got.reshape(rows - 1, t, wide)
        for r in range(1, rows):
            oa_copy(k, r).start()
        all_here(step_sem.at[5, k], hb.at[rest_cols, tok(k)])
        theirs = hb[rest_cols, tok(k)].reshape((cols - 1) * t, hidden)
        for j in range(wides):
            where = pl.ds(j * wide, wide)
            got = jnp.dot(theirs, wb[0, :, where], preferred_element_type=f32).astype(bf16)
            ob[0, :, tok(k), where] = got.reshape(cols - 1, t, wide)
        for c in range(1, cols):
            ob_copy(k, c).start()

    def local():
        def columns_of(j, _):
            where = pl.ds(pl.multiple_of(j * wide, wide), wide)
            for side, w in ((0, wa), (1, wb)):
                out_ref[:, columns((row, col), side, j * wide, wide)] = jnp.dot(
                    ha[0], w[0, :, where], preferred_element_type=f32
                ).astype(bf16)
            return 0

        lax.fori_loop(0, wides, columns_of, 0)

    def fetched_a(i):
        c, j = 1 + i // out_tiles, lax.rem(i, out_tiles)
        where = pl.ds(pl.multiple_of(j * out_tile, out_tile), out_tile)
        got = jnp.dot(
            ha[...].reshape(rows * count, hidden), wa[c, :, where], preferred_element_type=f32
        ).astype(bf16)
        oa[c, :, :, where] = got[count:].reshape(rows - 1, count, out_tile)
        for r in range(1, rows):
            ga_copy(c, j, r).start()
        out_ref[:, columns(up(0, c), 0, j * out_tile, out_tile)] = got[:count]

    def fetched_b(i):
        r, j = 1 + i // out_tiles, lax.rem(i, out_tiles)
        where = pl.ds(pl.multiple_of(j * out_tile, out_tile), out_tile)
        got = jnp.dot(
            hb[...].reshape(cols * count, hidden), wb[r, :, where], preferred_element_type=f32
        ).astype(bf16)
        ob[r, :, :, where] = got[count:].reshape(cols - 1, count, out_tile)
        for c in range(1, cols):
            gb_copy(r, j, c).start()
        out_ref[:, columns(up(r, 0), 1, j * out_tile, out_tile)] = got[:count]

    tiles_a, tiles_b = (cols - 1) * out_tiles, (rows - 1) * out_tiles
    both = min(tiles_a, tiles_b)

    def emit_fetched():
        def pair(i, _):
            fetched_a(i)
            fetched_b(i)
            return 0

        def only(one):
            def body(i, _):
                one(i)
                return 0

            return body

        lax.fori_loop(0, both, pair, 0)
        lax.fori_loop(both, tiles_a, only(fetched_a), 0)
        lax.fori_loop(both, tiles_b, only(fetched_b), 0)

    stages = {"project": project, "combine": combine, "activate": activate, "emit": emit}
    once = {
        "fetch": fetch, "last hops": last_hops, "landed": landed, "local": local, "emit fetched": emit_fetched,
    }
    for task in ORDER:
        if task in once:
            once[task]()
        else:
            name, at = task.split()
            if name == "hop":
                if int(at) < planes:
                    hop(int(at))
            else:
                stages[name](int(at))

    all_sent(X, xbuf.at[:, pl.ds(t, (n - 1) * t)])
    all_sent(A, rec_a.at[:, rest_rows])
    all_sent(B, rec_b.at[:, rest_cols])
    all_sent(C, fin_a.at[:, rest_cols])
    all_sent(D, fin_b.at[:, rest_rows])
    all_sent(HA, ha.at[rest_rows])
    all_sent(HB, hb.at[rest_cols])
    all_sent(FA, wa.at[rest_cols, own_share])
    all_sent(FB, wb.at[rest_rows, own_share])
    for side, (ref, rest) in enumerate(sides):
        all_sent(MA + side, ref.at[rest, pl.ds(0, planes * share)])
        if planes > 1:
            inner = jnp.logical_and(plane > 0, plane + 1 < planes)
            pl.when(inner)(lambda: all_sent(ZA + side, ref.at[rest, pl.ds(0, (planes + 1) * share)]))
            pl.when(jnp.logical_not(inner))(lambda: all_sent(ZA + side, ref.at[rest, pl.ds(0, share)]))
    all_sent(OA, oa)
    all_sent(OB, ob)
    all_here(out_sem.at[0], oa)
    all_here(out_sem.at[1], ob)


def solution(mesh):
    groups, rows, cols = mesh.shape["dp"], mesh.shape["row"], mesh.shape["col"]
    planes = groups // 2
    n = rows * cols

    def shards(tokens, w_gate, w_up, w_down):
        count, width = tokens.shape
        features, hidden = w_gate.shape
        side_cols = w_down.shape[1] // 2
        chunks = CHUNKS
        t = count // chunks
        bf16 = jnp.bfloat16
        any_space = pl.BlockSpec(memory_space=pl.ANY)
        dma = pltpu.SemaphoreType.DMA

        return pl.pallas_call(
            functools.partial(kernel, groups, rows, cols, chunks),
            out_shape=pltpu.VMEM((count, width), bf16),
            in_specs=[any_space] * 4,
            out_specs=pl.BlockSpec(memory_space=pltpu.VMEM),
            scratch_shapes=[
                pltpu.VMEM((count, width), bf16),
                pltpu.VMEM((2, hidden // groups, side_cols), bf16),
                pltpu.VMEM((features, hidden), bf16),
                pltpu.VMEM((features, hidden), bf16),
                pltpu.VMEM((cols, hidden, side_cols), bf16),
                pltpu.VMEM((rows, hidden, side_cols), bf16),
                pltpu.VMEM((chunks, n * t, features), bf16),
                pltpu.VMEM((chunks, 2, t, hidden), jnp.float32),
                pltpu.VMEM((chunks, 2, rows, cols, t, hidden), bf16),
                pltpu.VMEM((chunks, rows, cols, t, hidden), bf16),
                pltpu.VMEM((chunks, cols, rows, t, hidden), bf16),
                pltpu.VMEM((chunks, cols, t, hidden), bf16),
                pltpu.VMEM((chunks, rows, t, hidden), bf16),
                pltpu.VMEM((chunks, cols, t, hidden), bf16),
                pltpu.VMEM((chunks, rows, t, hidden), bf16),
                pltpu.VMEM((rows, count, hidden), bf16),
                pltpu.VMEM((cols, count, hidden), bf16),
                pltpu.VMEM((cols, rows - 1, count, side_cols), bf16),
                pltpu.VMEM((rows, cols - 1, count, side_cols), bf16),
                dma((7 + chunks,)),
                dma((15,)),
                dma((chunks,)),
                dma((6, chunks)),
                dma((2,)),
                dma((planes, 2)),
                dma((2,)),
                dma((2,)),
            ],
            compiler_params=pltpu.CompilerParams(collective_id=0, has_side_effects=True),
        )(tokens, w_gate, w_up, w_down)

    in_specs = (
        P(("dp", "row", "col"), None),
        P(("row", "col"), None),
        P(("row", "col"), None),
        P(None, ("row", "col")),
    )
    out_specs = P(("dp", "row", "col"), None)
    return jax.shard_map(shards, mesh=mesh, in_specs=in_specs, out_specs=out_specs, check_vma=False)
```

```python
import functools

import jax
import jax.numpy as jnp
from jax import lax
from jax.experimental import pallas as pl
from jax.experimental.pallas import tpu as pltpu
from jax.sharding import PartitionSpec as P

MESH = pl.DeviceIdType.MESH
CHUNKS = 4
EARLY_HOPS = 2
ORDER = (
    "fetch", "project 0", "project 1", "hop 1", "project 2", "project 3", "hop 2", "combine 0", "combine 1",
    "combine 2", "combine 3", "activate 0", "activate 1", "activate 2", "activate 3", "emit 0", "emit 1",
    "last hops", "local", "emit 2", "emit 3", "landed", "emit fetched",
)
X, A, B, C, D, HA, HB, OA, OB, FA, FB, ZA, ZB, MA, MB = range(15)


def tile_of(width, most):
    tile = min(width, most)
    while width % tile:
        tile //= 2
    return tile


def kernel(
    groups, rows, cols, chunks,
    x_ref, wg_ref, wu_ref, wd_ref, out_ref,
    xin, wf, wg, wu, wa, wb, xbuf, acc, part, rec_a, rec_b, sum_a, sum_b, fin_a, fin_b, ha, hb, oa, ob,
    load_sem, sent_sem, x_sem, step_sem, fetch_sem, land_sem, mate_sem, out_sem,
):
    n = rows * cols
    row, col = lax.axis_index("row"), lax.axis_index("col")
    group = lax.axis_index("dp")
    mates = 2
    planes = groups // mates
    plane, core = group // mates, lax.rem(group, mates)
    count = x_ref.shape[0]
    t = count // chunks
    features, hidden = wg.shape
    half = hidden // 2
    side_cols = wa.shape[2]
    share = hidden // groups
    bf16, f32 = jnp.bfloat16, jnp.float32

    def up(r, c):
        return lax.rem(row + r, rows), lax.rem(col + c, cols)

    def down(r, c):
        return lax.rem(row + rows - r, rows), lax.rem(col + cols - c, cols)

    def shard(rc, width):
        return pl.ds(pl.multiple_of((rc[0] * cols + rc[1]) * width, width), width)

    def remote(src, dst, kind, landing, to):
        return pltpu.make_async_remote_copy(
            src_ref=src, dst_ref=dst, send_sem=sent_sem.at[kind], recv_sem=landing,
            device_id={"row": to[0], "col": to[1]}, device_id_type=MESH,
        )

    def all_sent(kind, ref):
        remote(ref, ref, kind, out_sem.at[0], up(rows - 1, cols - 1)).wait_send()

    def all_here(landing, ref):
        remote(ref, ref, 0, landing, up(rows - 1, cols - 1)).wait_recv()

    def tok(k):
        return pl.ds(k * t, t)

    others = [(r, c) for r in range(rows) for c in range(cols)][1:]
    by_reach = others[::-1]
    rest_rows, rest_cols = pl.ds(1, rows - 1), pl.ds(1, cols - 1)

    def x_copy(k, r, c):
        to = up(r, c)
        return remote(
            xin.at[tok(k), shard(to, features)], xbuf.at[k, pl.ds((r * cols + c) * t, t)], X, x_sem.at[k], to
        )

    def a_copy(k, r):
        return remote(part.at[k, 0, r], rec_a.at[k, r], A, step_sem.at[0, k], down(r, 0))

    def b_copy(k, c):
        return remote(part.at[k, 1, :, c], rec_b.at[k, c], B, step_sem.at[1, k], down(0, c))

    def c_copy(k, c):
        return remote(sum_a.at[k, c], fin_a.at[k, c], C, step_sem.at[2, k], down(0, c))

    def d_copy(k, r):
        return remote(sum_b.at[k, r], fin_b.at[k, r], D, step_sem.at[3, k], down(r, 0))

    def ha_copy(k, r):
        return remote(ha.at[0, tok(k)], ha.at[r, tok(k)], HA, step_sem.at[4, k], up(r, 0))

    def hb_copy(k, c):
        return remote(hb.at[0, tok(k)], hb.at[c, tok(k)], HB, step_sem.at[5, k], up(0, c))

    def share_of(g):
        return pl.ds(pl.multiple_of(g * share, share), share)

    def fetch_a(c):
        return remote(wf.at[0], wa.at[c, share_of(group)], FA, fetch_sem.at[0], down(0, c))

    def fetch_b(r):
        return remote(wf.at[1], wb.at[r, share_of(group)], FB, fetch_sem.at[1], down(r, 0))

    sides = ((wa, rest_cols), (wb, rest_rows))

    def pass_on(source, side, to_plane):
        ref, rest = sides[side]
        region = ref.at[rest, share_of(source * mates + core)]
        return pltpu.make_async_remote_copy(
            src_ref=region, dst_ref=region, send_sem=sent_sem.at[ZA + side], recv_sem=land_sem.at[source, side],
            device_id={"dp": to_plane * mates + core}, device_id_type=MESH,
        )

    def to_mate(source, side):
        ref, rest = sides[side]
        region = ref.at[rest, share_of(source * mates + core)]
        return pltpu.make_async_remote_copy(
            src_ref=region, dst_ref=region, send_sem=sent_sem.at[MA + side], recv_sem=mate_sem.at[side],
            device_id={"dp": plane * mates + (mates - 1 - core)}, device_id_type=MESH,
        )

    def spread(source, side, upward, downward):
        if upward:
            pl.when(plane + 1 < planes)(lambda: pass_on(source, side, plane + 1).start())
        if downward:
            pl.when(plane > 0)(lambda: pass_on(source, side, plane - 1).start())
        to_mate(source, side).start()

    def hop(h):
        below, above = plane - h, plane + h
        for side in range(2):

            @pl.when(below >= 0)
            def _():
                pass_on(below, side, plane).wait_recv()
                spread(below, side, True, False)

            @pl.when(above < planes)
            def _():
                pass_on(above, side, plane).wait_recv()
                spread(above, side, False, True)

    def last_hops():
        def more(h, _):
            hop(h)
            return 0

        lax.fori_loop(EARLY_HOPS + 1, planes, more, 0)

    def landed():
        for side, (ref, rest) in enumerate(sides):
            all_here(mate_sem.at[side], ref.at[rest, pl.ds(0, planes * share)])

    def columns(rc, side, start, width):
        base = (rc[0] * cols + rc[1]) * 2 * side_cols + side * side_cols + start
        return pl.ds(pl.multiple_of(base, width), width)

    def oa_copy(k, r):
        return remote(
            oa.at[0, r - 1, tok(k)], out_ref.at[tok(k), columns((row, col), 0, 0, side_cols)],
            OA, out_sem.at[0], down(r, 0),
        )

    def ob_copy(k, c):
        return remote(
            ob.at[0, c - 1, tok(k)], out_ref.at[tok(k), columns((row, col), 1, 0, side_cols)],
            OB, out_sem.at[1], down(0, c),
        )

    out_tile = tile_of(side_cols, 256)
    out_tiles = side_cols // out_tile

    def ga_copy(c, j, r):
        return remote(
            oa.at[c, r - 1, :, pl.ds(pl.multiple_of(j * out_tile, out_tile), out_tile)],
            out_ref.at[:, columns(up(0, c), 0, j * out_tile, out_tile)],
            OA, out_sem.at[0], down(r, 0),
        )

    def gb_copy(r, j, c):
        return remote(
            ob.at[r, c - 1, :, pl.ds(pl.multiple_of(j * out_tile, out_tile), out_tile)],
            out_ref.at[:, columns(up(r, 0), 1, j * out_tile, out_tile)],
            OB, out_sem.at[1], down(0, c),
        )

    own_share = share_of(group)
    first_loads = [
        pltpu.make_async_copy(wd_ref.at[own_share, pl.ds(0, side_cols)], wf.at[0], load_sem.at[0]),
        pltpu.make_async_copy(wd_ref.at[own_share, pl.ds(side_cols, side_cols)], wf.at[1], load_sem.at[1]),
        pltpu.make_async_copy(x_ref, xin, load_sem.at[2]),
    ]
    own = [
        pltpu.make_async_copy(
            x_ref.at[tok(k), shard((row, col), features)], xbuf.at[k, pl.ds(0, t)], load_sem.at[3 + k]
        )
        for k in range(chunks)
    ]
    loads = [
        pltpu.make_async_copy(wg_ref, wg, load_sem.at[3 + chunks]),
        pltpu.make_async_copy(wu_ref, wu, load_sem.at[4 + chunks]),
        pltpu.make_async_copy(wd_ref.at[:, pl.ds(0, side_cols)], wa.at[0], load_sem.at[5 + chunks]),
        pltpu.make_async_copy(wd_ref.at[:, pl.ds(side_cols, side_cols)], wb.at[0], load_sem.at[6 + chunks]),
    ]

    for load in first_loads:
        load.start()

    barrier = pltpu.get_barrier_semaphore()
    for r, c in others:
        to = up(r, c)
        pl.semaphore_signal(barrier, inc=1, device_id={"row": to[0], "col": to[1]}, device_id_type=MESH)

    def greet(g):
        pl.semaphore_signal(barrier, inc=1, device_id={"dp": g}, device_id_type=MESH)

    pl.when(plane > 0)(lambda: greet(group - mates))
    pl.when(plane + 1 < planes)(lambda: greet(group + mates))
    greet(plane * mates + (mates - 1 - core))
    neighbours = (plane > 0).astype(jnp.int32) + (plane + 1 < planes).astype(jnp.int32)
    for load in first_loads[:2]:
        load.wait()
    pl.semaphore_wait(barrier, n - 1 + mates - 1 + neighbours)

    for c in range(1, cols):
        fetch_a(c).start()
    for r in range(1, rows):
        fetch_b(r).start()
    first_loads[2].wait()
    for k in range(chunks):
        for r, c in by_reach:
            x_copy(k, r, c).start()
    for load in own + loads:
        load.start()

    def fetch():
        all_here(fetch_sem.at[0], wa.at[rest_cols, own_share])
        spread(plane, 0, True, True)
        all_here(fetch_sem.at[1], wb.at[rest_rows, own_share])
        spread(plane, 1, True, True)
        for load in loads:
            load.wait()

    tile = tile_of(half, 512)
    per_half = half // tile

    def project(k):
        own[k].wait()
        all_here(x_sem.at[k], xbuf.at[k, pl.ds(t, (n - 1) * t)])

        def column(j, _):
            side, at = j // per_half, lax.rem(j, per_half) * tile
            source = pl.ds(pl.multiple_of(j * tile, tile), tile)
            for w, base in ((wg, 0), (wu, half)):
                target = pl.ds(pl.multiple_of(base + at, tile), tile)
                got = jnp.dot(xbuf[k], w[:, source], preferred_element_type=f32)
                acc[k, side, :, target] = got[:t]
                for r, c in others:
                    first = (r * cols + c) * t
                    part[k, side, r, c, :, target] = got[first : first + t].astype(bf16)
            return 0

        lax.fori_loop(0, 2 * per_half, column, 0)
        for r in range(1, rows):
            a_copy(k, r).start()
        for c in range(1, cols):
            b_copy(k, c).start()

    def combine(k):
        all_here(step_sem.at[0, k], rec_a.at[k, rest_rows])
        for c in range(1, cols):
            total = part[k, 0, 0, c].astype(f32)
            for r in range(1, rows):
                total = total + rec_a[k, r, c].astype(f32)
            sum_a[k, c] = total.astype(bf16)
            c_copy(k, c).start()
        all_here(step_sem.at[1, k], rec_b.at[k, rest_cols])
        for r in range(1, rows):
            total = part[k, 1, r, 0].astype(f32)
            for c in range(1, cols):
                total = total + rec_b[k, c, r].astype(f32)
            sum_b[k, r] = total.astype(bf16)
            d_copy(k, r).start()

    def activate(k):
        all_here(step_sem.at[2, k], fin_a.at[k, rest_cols])
        all_here(step_sem.at[3, k], fin_b.at[k, rest_rows])
        for side in range(2):
            total = acc[k, side]
            if side == 0:
                for r in range(1, rows):
                    total = total + rec_a[k, r, 0].astype(f32)
                for c in range(1, cols):
                    total = total + fin_a[k, c].astype(f32)
            else:
                for c in range(1, cols):
                    total = total + rec_b[k, c, 0].astype(f32)
                for r in range(1, rows):
                    total = total + fin_b[k, r].astype(f32)
            gate = total[:, :half]
            done = (gate / (1.0 + jnp.exp(-gate)) * total[:, half:]).astype(bf16)
            ha[0, tok(k), pl.ds(side * half, half)] = done
            hb[0, tok(k), pl.ds(side * half, half)] = done
        for r in range(1, rows):
            ha_copy(k, r).start()
        for c in range(1, cols):
            hb_copy(k, c).start()

    wide = tile_of(side_cols, 512)
    wides = side_cols // wide

    def emit(k):
        all_here(step_sem.at[4, k], ha.at[rest_rows, tok(k)])
        theirs = ha[rest_rows, tok(k)].reshape((rows - 1) * t, hidden)
        for j in range(wides):
            where = pl.ds(j * wide, wide)
            got = jnp.dot(theirs, wa[0, :, where], preferred_element_type=f32).astype(bf16)
            oa[0, :, tok(k), where] = got.reshape(rows - 1, t, wide)
        for r in range(1, rows):
            oa_copy(k, r).start()
        all_here(step_sem.at[5, k], hb.at[rest_cols, tok(k)])
        theirs = hb[rest_cols, tok(k)].reshape((cols - 1) * t, hidden)
        for j in range(wides):
            where = pl.ds(j * wide, wide)
            got = jnp.dot(theirs, wb[0, :, where], preferred_element_type=f32).astype(bf16)
            ob[0, :, tok(k), where] = got.reshape(cols - 1, t, wide)
        for c in range(1, cols):
            ob_copy(k, c).start()

    def local():
        def columns_of(j, _):
            where = pl.ds(pl.multiple_of(j * wide, wide), wide)
            for side, w in ((0, wa), (1, wb)):
                out_ref[:, columns((row, col), side, j * wide, wide)] = jnp.dot(
                    ha[0], w[0, :, where], preferred_element_type=f32
                ).astype(bf16)
            return 0

        lax.fori_loop(0, wides, columns_of, 0)

    def fetched_a(i):
        c, j = 1 + i // out_tiles, lax.rem(i, out_tiles)
        where = pl.ds(pl.multiple_of(j * out_tile, out_tile), out_tile)
        got = jnp.dot(
            ha[...].reshape(rows * count, hidden), wa[c, :, where], preferred_element_type=f32
        ).astype(bf16)
        oa[c, :, :, where] = got[count:].reshape(rows - 1, count, out_tile)
        for r in range(1, rows):
            ga_copy(c, j, r).start()
        out_ref[:, columns(up(0, c), 0, j * out_tile, out_tile)] = got[:count]

    def fetched_b(i):
        r, j = 1 + i // out_tiles, lax.rem(i, out_tiles)
        where = pl.ds(pl.multiple_of(j * out_tile, out_tile), out_tile)
        got = jnp.dot(
            hb[...].reshape(cols * count, hidden), wb[r, :, where], preferred_element_type=f32
        ).astype(bf16)
        ob[r, :, :, where] = got[count:].reshape(cols - 1, count, out_tile)
        for c in range(1, cols):
            gb_copy(r, j, c).start()
        out_ref[:, columns(up(r, 0), 1, j * out_tile, out_tile)] = got[:count]

    tiles_a, tiles_b = (cols - 1) * out_tiles, (rows - 1) * out_tiles
    both = min(tiles_a, tiles_b)

    def emit_fetched():
        def pair(i, _):
            fetched_a(i)
            fetched_b(i)
            return 0

        def only(one):
            def body(i, _):
                one(i)
                return 0

            return body

        lax.fori_loop(0, both, pair, 0)
        lax.fori_loop(both, tiles_a, only(fetched_a), 0)
        lax.fori_loop(both, tiles_b, only(fetched_b), 0)

    stages = {"project": project, "combine": combine, "activate": activate, "emit": emit}
    once = {
        "fetch": fetch, "last hops": last_hops, "landed": landed, "local": local, "emit fetched": emit_fetched,
    }
    for task in ORDER:
        if task in once:
            once[task]()
        else:
            name, at = task.split()
            if name == "hop":
                if int(at) < planes:
                    hop(int(at))
            else:
                stages[name](int(at))

    all_sent(X, xbuf.at[:, pl.ds(t, (n - 1) * t)])
    all_sent(A, rec_a.at[:, rest_rows])
    all_sent(B, rec_b.at[:, rest_cols])
    all_sent(C, fin_a.at[:, rest_cols])
    all_sent(D, fin_b.at[:, rest_rows])
    all_sent(HA, ha.at[rest_rows])
    all_sent(HB, hb.at[rest_cols])
    all_sent(FA, wa.at[rest_cols, own_share])
    all_sent(FB, wb.at[rest_rows, own_share])
    for side, (ref, rest) in enumerate(sides):
        all_sent(MA + side, ref.at[rest, pl.ds(0, planes * share)])
        if planes > 1:
            inner = jnp.logical_and(plane > 0, plane + 1 < planes)
            pl.when(inner)(lambda: all_sent(ZA + side, ref.at[rest, pl.ds(0, (planes + 1) * share)]))
            pl.when(jnp.logical_not(inner))(lambda: all_sent(ZA + side, ref.at[rest, pl.ds(0, share)]))
    all_sent(OA, oa)
    all_sent(OB, ob)
    all_here(out_sem.at[0], oa)
    all_here(out_sem.at[1], ob)


def solution(mesh):
    groups, rows, cols = mesh.shape["dp"], mesh.shape["row"], mesh.shape["col"]
    planes = groups // 2
    n = rows * cols

    def shards(tokens, w_gate, w_up, w_down):
        count, width = tokens.shape
        features, hidden = w_gate.shape
        side_cols = w_down.shape[1] // 2
        chunks = CHUNKS
        t = count // chunks
        bf16 = jnp.bfloat16
        any_space = pl.BlockSpec(memory_space=pl.ANY)
        dma = pltpu.SemaphoreType.DMA

        return pl.pallas_call(
            functools.partial(kernel, groups, rows, cols, chunks),
            out_shape=pltpu.VMEM((count, width), bf16),
            in_specs=[any_space] * 4,
            out_specs=pl.BlockSpec(memory_space=pltpu.VMEM),
            scratch_shapes=[
                pltpu.VMEM((count, width), bf16),
                pltpu.VMEM((2, hidden // groups, side_cols), bf16),
                pltpu.VMEM((features, hidden), bf16),
                pltpu.VMEM((features, hidden), bf16),
                pltpu.VMEM((cols, hidden, side_cols), bf16),
                pltpu.VMEM((rows, hidden, side_cols), bf16),
                pltpu.VMEM((chunks, n * t, features), bf16),
                pltpu.VMEM((chunks, 2, t, hidden), jnp.float32),
                pltpu.VMEM((chunks, 2, rows, cols, t, hidden), bf16),
                pltpu.VMEM((chunks, rows, cols, t, hidden), bf16),
                pltpu.VMEM((chunks, cols, rows, t, hidden), bf16),
                pltpu.VMEM((chunks, cols, t, hidden), bf16),
                pltpu.VMEM((chunks, rows, t, hidden), bf16),
                pltpu.VMEM((chunks, cols, t, hidden), bf16),
                pltpu.VMEM((chunks, rows, t, hidden), bf16),
                pltpu.VMEM((rows, count, hidden), bf16),
                pltpu.VMEM((cols, count, hidden), bf16),
                pltpu.VMEM((cols, rows - 1, count, side_cols), bf16),
                pltpu.VMEM((rows, cols - 1, count, side_cols), bf16),
                dma((7 + chunks,)),
                dma((15,)),
                dma((chunks,)),
                dma((6, chunks)),
                dma((2,)),
                dma((planes, 2)),
                dma((2,)),
                dma((2,)),
            ],
            compiler_params=pltpu.CompilerParams(collective_id=0, has_side_effects=True),
        )(tokens, w_gate, w_up, w_down)

    in_specs = (
        P(("dp", "row", "col"), None),
        P(("row", "col"), None),
        P(("row", "col"), None),
        P(None, ("row", "col")),
    )
    out_specs = P(("dp", "row", "col"), None)
    return jax.shard_map(shards, mesh=mesh, in_specs=in_specs, out_specs=out_specs, check_vma=False)
```

```python
import functools
import math

import jax
import jax.numpy as jnp
from jax import lax
from jax.experimental import pallas as pl
from jax.experimental.pallas import tpu as pltpu
from jax.sharding import PartitionSpec as P

MESH = pl.DeviceIdType.MESH
CHUNKS = 4
SMALL_PART = 5, 16
EARLY_HOPS = 2
ORDER = (
    "fetch", "project 0", "project 1", "hop 1", "project 2", "project 3", "hop 2", "combine 0", "combine 1",
    "combine 2", "combine 3", "activate 0", "activate 1", "activate 2", "activate 3", "emit 0", "emit 1",
    "last hops", "local", "emit 2", "emit 3", "landed", "emit fetched",
)
X, A, B, C, D, HA, HB, OA, OB, FA, FB, ZA, ZB, MA, MB = range(15)


def tile_of(width, most):
    tile = min(width, most)
    while width % tile:
        tile //= 2
    return tile


def small_share(pair):
    return max(16, pair * SMALL_PART[0] // SMALL_PART[1] // 16 * 16)


def kernel(
    groups, rows, cols, chunks,
    x_ref, wg_ref, wu_ref, wd_ref, out_ref,
    xin, wf, wg, wu, wa, wb, xbuf, acc, part, rec_a, rec_b, sum_a, sum_b, fin_a, fin_b, ha, hb, oa, ob,
    load_sem, sent_sem, x_sem, step_sem, fetch_sem, land_sem, mate_sem, out_sem,
):
    n = rows * cols
    row, col = lax.axis_index("row"), lax.axis_index("col")
    group = lax.axis_index("dp")
    mates = 2
    planes = groups // mates
    plane, core = group // mates, lax.rem(group, mates)
    count = x_ref.shape[0]
    t = count // chunks
    features, hidden = wg.shape
    half = hidden // 2
    side_cols = wa.shape[2]
    pair = mates * hidden // groups
    small = small_share(pair)
    bf16, f32 = jnp.bfloat16, jnp.float32

    def up(r, c):
        return lax.rem(row + r, rows), lax.rem(col + c, cols)

    def down(r, c):
        return lax.rem(row + rows - r, rows), lax.rem(col + cols - c, cols)

    def shard(rc, width):
        return pl.ds(pl.multiple_of((rc[0] * cols + rc[1]) * width, width), width)

    def remote(src, dst, kind, landing, to):
        return pltpu.make_async_remote_copy(
            src_ref=src, dst_ref=dst, send_sem=sent_sem.at[kind], recv_sem=landing,
            device_id={"row": to[0], "col": to[1]}, device_id_type=MESH,
        )

    def all_sent(kind, ref):
        remote(ref, ref, kind, out_sem.at[0], up(rows - 1, cols - 1)).wait_send()

    def all_here(landing, ref):
        remote(ref, ref, 0, landing, up(rows - 1, cols - 1)).wait_recv()

    def tok(k):
        return pl.ds(k * t, t)

    others = [(r, c) for r in range(rows) for c in range(cols)][1:]
    by_reach = others[::-1]
    rest_rows, rest_cols = pl.ds(1, rows - 1), pl.ds(1, cols - 1)

    def x_copy(k, r, c):
        to = up(r, c)
        return remote(
            xin.at[tok(k), shard(to, features)], xbuf.at[k, pl.ds((r * cols + c) * t, t)], X, x_sem.at[k], to
        )

    def a_copy(k, r):
        return remote(part.at[k, 0, r], rec_a.at[k, r], A, step_sem.at[0, k], down(r, 0))

    def b_copy(k, c):
        return remote(part.at[k, 1, :, c], rec_b.at[k, c], B, step_sem.at[1, k], down(0, c))

    def c_copy(k, c):
        return remote(sum_a.at[k, c], fin_a.at[k, c], C, step_sem.at[2, k], down(0, c))

    def d_copy(k, r):
        return remote(sum_b.at[k, r], fin_b.at[k, r], D, step_sem.at[3, k], down(r, 0))

    def ha_copy(k, r):
        return remote(ha.at[0, tok(k)], ha.at[r, tok(k)], HA, step_sem.at[4, k], up(r, 0))

    def hb_copy(k, c):
        return remote(hb.at[0, tok(k)], hb.at[c, tok(k)], HB, step_sem.at[5, k], up(0, c))

    share_sizes = (small, pair - small)

    def share_of(source, m):
        start = source * pair + (small if m else 0)
        return pl.ds(pl.multiple_of(start, math.gcd(pair, small)), share_sizes[m])

    def as_core(do):
        for m in range(mates):

            @pl.when(core == m)
            def _():
                do(m)

    def fetch_a(m, c):
        return remote(
            wf.at[0, pl.ds(0, share_sizes[m])], wa.at[c, share_of(plane, m)], FA, fetch_sem.at[0], down(0, c)
        )

    def fetch_b(m, r):
        return remote(
            wf.at[1, pl.ds(0, share_sizes[m])], wb.at[r, share_of(plane, m)], FB, fetch_sem.at[1], down(r, 0)
        )

    sides = ((wa, rest_cols), (wb, rest_rows))

    def pass_on(source, side, m, to_plane):
        ref, rest = sides[side]
        region = ref.at[rest, share_of(source, m)]
        return pltpu.make_async_remote_copy(
            src_ref=region, dst_ref=region, send_sem=sent_sem.at[ZA + side], recv_sem=land_sem.at[source, side],
            device_id={"dp": to_plane * mates + core}, device_id_type=MESH,
        )

    def to_mate(source, side, m):
        ref, rest = sides[side]
        region = ref.at[rest, share_of(source, m)]
        return pltpu.make_async_remote_copy(
            src_ref=region, dst_ref=region, send_sem=sent_sem.at[MA + side], recv_sem=mate_sem.at[side],
            device_id={"dp": plane * mates + (mates - 1 - core)}, device_id_type=MESH,
        )

    def spread(source, side, m, upward, downward):
        if upward:
            pl.when(plane + 1 < planes)(lambda: pass_on(source, side, m, plane + 1).start())
        if downward:
            pl.when(plane > 0)(lambda: pass_on(source, side, m, plane - 1).start())
        to_mate(source, side, m).start()

    def hop(h):
        below, above = plane - h, plane + h

        def relay(m):
            for side in range(2):

                @pl.when(below >= 0)
                def _():
                    pass_on(below, side, m, plane).wait_recv()
                    spread(below, side, m, True, False)

                @pl.when(above < planes)
                def _():
                    pass_on(above, side, m, plane).wait_recv()
                    spread(above, side, m, False, True)

        as_core(relay)

    def last_hops():
        def more(h, _):
            hop(h)
            return 0

        lax.fori_loop(EARLY_HOPS + 1, planes, more, 0)

    def landed():
        def from_mate(m):
            for side, (ref, rest) in enumerate(sides):
                all_here(mate_sem.at[side], ref.at[rest, pl.ds(0, planes * share_sizes[1 - m])])

        as_core(from_mate)

    def columns(rc, side, start, width):
        base = (rc[0] * cols + rc[1]) * 2 * side_cols + side * side_cols + start
        return pl.ds(pl.multiple_of(base, width), width)

    def oa_copy(k, r):
        return remote(
            oa.at[0, r - 1, tok(k)], out_ref.at[tok(k), columns((row, col), 0, 0, side_cols)],
            OA, out_sem.at[0], down(r, 0),
        )

    def ob_copy(k, c):
        return remote(
            ob.at[0, c - 1, tok(k)], out_ref.at[tok(k), columns((row, col), 1, 0, side_cols)],
            OB, out_sem.at[1], down(0, c),
        )

    out_tile = tile_of(side_cols, 256)
    out_tiles = side_cols // out_tile

    def ga_copy(c, j, r):
        return remote(
            oa.at[c, r - 1, :, pl.ds(pl.multiple_of(j * out_tile, out_tile), out_tile)],
            out_ref.at[:, columns(up(0, c), 0, j * out_tile, out_tile)],
            OA, out_sem.at[0], down(r, 0),
        )

    def gb_copy(r, j, c):
        return remote(
            ob.at[r, c - 1, :, pl.ds(pl.multiple_of(j * out_tile, out_tile), out_tile)],
            out_ref.at[:, columns(up(r, 0), 1, j * out_tile, out_tile)],
            OB, out_sem.at[1], down(0, c),
        )

    def load_share(m):
        return [
            pltpu.make_async_copy(
                wd_ref.at[share_of(plane, m), pl.ds(side * side_cols, side_cols)],
                wf.at[side, pl.ds(0, share_sizes[m])], load_sem.at[side],
            )
            for side in range(2)
        ]

    load_tokens = pltpu.make_async_copy(x_ref, xin, load_sem.at[2])
    own = [
        pltpu.make_async_copy(
            x_ref.at[tok(k), shard((row, col), features)], xbuf.at[k, pl.ds(0, t)], load_sem.at[3 + k]
        )
        for k in range(chunks)
    ]
    loads = [
        pltpu.make_async_copy(wg_ref, wg, load_sem.at[3 + chunks]),
        pltpu.make_async_copy(wu_ref, wu, load_sem.at[4 + chunks]),
        pltpu.make_async_copy(wd_ref.at[:, pl.ds(0, side_cols)], wa.at[0], load_sem.at[5 + chunks]),
        pltpu.make_async_copy(wd_ref.at[:, pl.ds(side_cols, side_cols)], wb.at[0], load_sem.at[6 + chunks]),
    ]

    as_core(lambda m: [load.start() for load in load_share(m)])
    load_tokens.start()

    barrier = pltpu.get_barrier_semaphore()
    for r, c in others:
        to = up(r, c)
        pl.semaphore_signal(barrier, inc=1, device_id={"row": to[0], "col": to[1]}, device_id_type=MESH)

    def greet(g):
        pl.semaphore_signal(barrier, inc=1, device_id={"dp": g}, device_id_type=MESH)

    pl.when(plane > 0)(lambda: greet(group - mates))
    pl.when(plane + 1 < planes)(lambda: greet(group + mates))
    greet(plane * mates + (mates - 1 - core))
    neighbours = (plane > 0).astype(jnp.int32) + (plane + 1 < planes).astype(jnp.int32)
    as_core(lambda m: [load.wait() for load in load_share(m)])
    pl.semaphore_wait(barrier, n - 1 + mates - 1 + neighbours)

    def send_share(m):
        for c in range(1, cols):
            fetch_a(m, c).start()
        for r in range(1, rows):
            fetch_b(m, r).start()

    as_core(send_share)
    load_tokens.wait()
    for k in range(chunks):
        for r, c in by_reach:
            x_copy(k, r, c).start()
    for load in own + loads:
        load.start()

    def fetch():
        def take(m):
            for side, (ref, rest) in enumerate(sides):
                all_here(fetch_sem.at[side], ref.at[rest, share_of(plane, m)])
                spread(plane, side, m, True, True)

        as_core(take)
        for load in loads:
            load.wait()

    tile = tile_of(half, 512)
    per_half = half // tile

    def project(k):
        own[k].wait()
        all_here(x_sem.at[k], xbuf.at[k, pl.ds(t, (n - 1) * t)])

        def column(j, _):
            side, at = j // per_half, lax.rem(j, per_half) * tile
            source = pl.ds(pl.multiple_of(j * tile, tile), tile)
            for w, base in ((wg, 0), (wu, half)):
                target = pl.ds(pl.multiple_of(base + at, tile), tile)
                got = jnp.dot(xbuf[k], w[:, source], preferred_element_type=f32)
                acc[k, side, :, target] = got[:t]
                for r, c in others:
                    first = (r * cols + c) * t
                    part[k, side, r, c, :, target] = got[first : first + t].astype(bf16)
            return 0

        lax.fori_loop(0, 2 * per_half, column, 0)
        for r in range(1, rows):
            a_copy(k, r).start()
        for c in range(1, cols):
            b_copy(k, c).start()

    def combine(k):
        all_here(step_sem.at[0, k], rec_a.at[k, rest_rows])
        for c in range(1, cols):
            total = part[k, 0, 0, c].astype(f32)
            for r in range(1, rows):
                total = total + rec_a[k, r, c].astype(f32)
            sum_a[k, c] = total.astype(bf16)
            c_copy(k, c).start()
        all_here(step_sem.at[1, k], rec_b.at[k, rest_cols])
        for r in range(1, rows):
            total = part[k, 1, r, 0].astype(f32)
            for c in range(1, cols):
                total = total + rec_b[k, c, r].astype(f32)
            sum_b[k, r] = total.astype(bf16)
            d_copy(k, r).start()

    def activate(k):
        all_here(step_sem.at[2, k], fin_a.at[k, rest_cols])
        all_here(step_sem.at[3, k], fin_b.at[k, rest_rows])
        for side in range(2):
            total = acc[k, side]
            if side == 0:
                for r in range(1, rows):
                    total = total + rec_a[k, r, 0].astype(f32)
                for c in range(1, cols):
                    total = total + fin_a[k, c].astype(f32)
            else:
                for c in range(1, cols):
                    total = total + rec_b[k, c, 0].astype(f32)
                for r in range(1, rows):
                    total = total + fin_b[k, r].astype(f32)
            gate = total[:, :half]
            done = (gate / (1.0 + jnp.exp(-gate)) * total[:, half:]).astype(bf16)
            ha[0, tok(k), pl.ds(side * half, half)] = done
            hb[0, tok(k), pl.ds(side * half, half)] = done
        for r in range(1, rows):
            ha_copy(k, r).start()
        for c in range(1, cols):
            hb_copy(k, c).start()

    wide = tile_of(side_cols, 512)
    wides = side_cols // wide

    def emit(k):
        all_here(step_sem.at[4, k], ha.at[rest_rows, tok(k)])
        theirs = ha[rest_rows, tok(k)].reshape((rows - 1) * t, hidden)
        for j in range(wides):
            where = pl.ds(j * wide, wide)
            got = jnp.dot(theirs, wa[0, :, where], preferred_element_type=f32).astype(bf16)
            oa[0, :, tok(k), where] = got.reshape(rows - 1, t, wide)
        for r in range(1, rows):
            oa_copy(k, r).start()
        all_here(step_sem.at[5, k], hb.at[rest_cols, tok(k)])
        theirs = hb[rest_cols, tok(k)].reshape((cols - 1) * t, hidden)
        for j in range(wides):
            where = pl.ds(j * wide, wide)
            got = jnp.dot(theirs, wb[0, :, where], preferred_element_type=f32).astype(bf16)
            ob[0, :, tok(k), where] = got.reshape(cols - 1, t, wide)
        for c in range(1, cols):
            ob_copy(k, c).start()

    def local():
        def columns_of(j, _):
            where = pl.ds(pl.multiple_of(j * wide, wide), wide)
            for side, w in ((0, wa), (1, wb)):
                out_ref[:, columns((row, col), side, j * wide, wide)] = jnp.dot(
                    ha[0], w[0, :, where], preferred_element_type=f32
                ).astype(bf16)
            return 0

        lax.fori_loop(0, wides, columns_of, 0)

    def fetched_a(i):
        c, j = 1 + i // out_tiles, lax.rem(i, out_tiles)
        where = pl.ds(pl.multiple_of(j * out_tile, out_tile), out_tile)
        got = jnp.dot(
            ha[...].reshape(rows * count, hidden), wa[c, :, where], preferred_element_type=f32
        ).astype(bf16)
        oa[c, :, :, where] = got[count:].reshape(rows - 1, count, out_tile)
        out_ref[:, columns(up(0, c), 0, j * out_tile, out_tile)] = got[:count]
        for r in range(1, rows):
            ga_copy(c, j, r).start()

    def fetched_b(i):
        r, j = 1 + i // out_tiles, lax.rem(i, out_tiles)
        where = pl.ds(pl.multiple_of(j * out_tile, out_tile), out_tile)
        got = jnp.dot(
            hb[...].reshape(cols * count, hidden), wb[r, :, where], preferred_element_type=f32
        ).astype(bf16)
        ob[r, :, :, where] = got[count:].reshape(cols - 1, count, out_tile)
        out_ref[:, columns(up(r, 0), 1, j * out_tile, out_tile)] = got[:count]
        for c in range(1, cols):
            gb_copy(r, j, c).start()

    tiles_a, tiles_b = (cols - 1) * out_tiles, (rows - 1) * out_tiles
    both = min(tiles_a, tiles_b)

    def emit_fetched():
        def pair(i, _):
            fetched_a(i)
            fetched_b(i)
            return 0

        def only(one):
            def body(i, _):
                one(i)
                return 0

            return body

        lax.fori_loop(0, both, pair, 0)
        lax.fori_loop(both, tiles_a, only(fetched_a), 0)
        lax.fori_loop(both, tiles_b, only(fetched_b), 0)

    stages = {"project": project, "combine": combine, "activate": activate, "emit": emit}
    once = {
        "fetch": fetch, "last hops": last_hops, "landed": landed, "local": local, "emit fetched": emit_fetched,
    }
    for task in ORDER:
        if task in once:
            once[task]()
        else:
            name, at = task.split()
            if name == "hop":
                if int(at) < planes:
                    hop(int(at))
            else:
                stages[name](int(at))

    all_sent(X, xbuf.at[:, pl.ds(t, (n - 1) * t)])
    all_sent(A, rec_a.at[:, rest_rows])
    all_sent(B, rec_b.at[:, rest_cols])
    all_sent(C, fin_a.at[:, rest_cols])
    all_sent(D, fin_b.at[:, rest_rows])
    all_sent(HA, ha.at[rest_rows])
    all_sent(HB, hb.at[rest_cols])

    def shares_sent(m):
        size = share_sizes[m]
        for side, (ref, rest) in enumerate(sides):
            all_sent(FA + side, ref.at[rest, pl.ds(0, size)])
            all_sent(MA + side, ref.at[rest, pl.ds(0, planes * size)])
            if planes > 1:
                inner = jnp.logical_and(plane > 0, plane + 1 < planes)
                pl.when(inner)(lambda: all_sent(ZA + side, ref.at[rest, pl.ds(0, (planes + 1) * size)]))
                pl.when(jnp.logical_not(inner))(lambda: all_sent(ZA + side, ref.at[rest, pl.ds(0, size)]))

    as_core(shares_sent)
    all_sent(OA, oa)
    all_sent(OB, ob)
    all_here(out_sem.at[0], oa)
    all_here(out_sem.at[1], ob)


def solution(mesh):
    groups, rows, cols = mesh.shape["dp"], mesh.shape["row"], mesh.shape["col"]
    planes = groups // 2
    n = rows * cols

    def shards(tokens, w_gate, w_up, w_down):
        count, width = tokens.shape
        features, hidden = w_gate.shape
        side_cols = w_down.shape[1] // 2
        pair = 2 * hidden // groups
        chunks = CHUNKS
        t = count // chunks
        bf16 = jnp.bfloat16
        any_space = pl.BlockSpec(memory_space=pl.ANY)
        dma = pltpu.SemaphoreType.DMA

        return pl.pallas_call(
            functools.partial(kernel, groups, rows, cols, chunks),
            out_shape=pltpu.VMEM((count, width), bf16),
            in_specs=[any_space] * 4,
            out_specs=pl.BlockSpec(memory_space=pltpu.VMEM),
            scratch_shapes=[
                pltpu.VMEM((count, width), bf16),
                pltpu.VMEM((2, pair - small_share(pair), side_cols), bf16),
                pltpu.VMEM((features, hidden), bf16),
                pltpu.VMEM((features, hidden), bf16),
                pltpu.VMEM((cols, hidden, side_cols), bf16),
                pltpu.VMEM((rows, hidden, side_cols), bf16),
                pltpu.VMEM((chunks, n * t, features), bf16),
                pltpu.VMEM((chunks, 2, t, hidden), jnp.float32),
                pltpu.VMEM((chunks, 2, rows, cols, t, hidden), bf16),
                pltpu.VMEM((chunks, rows, cols, t, hidden), bf16),
                pltpu.VMEM((chunks, cols, rows, t, hidden), bf16),
                pltpu.VMEM((chunks, cols, t, hidden), bf16),
                pltpu.VMEM((chunks, rows, t, hidden), bf16),
                pltpu.VMEM((chunks, cols, t, hidden), bf16),
                pltpu.VMEM((chunks, rows, t, hidden), bf16),
                pltpu.VMEM((rows, count, hidden), bf16),
                pltpu.VMEM((cols, count, hidden), bf16),
                pltpu.VMEM((cols, rows - 1, count, side_cols), bf16),
                pltpu.VMEM((rows, cols - 1, count, side_cols), bf16),
                dma((7 + chunks,)),
                dma((15,)),
                dma((chunks,)),
                dma((6, chunks)),
                dma((2,)),
                dma((planes, 2)),
                dma((2,)),
                dma((2,)),
            ],
            compiler_params=pltpu.CompilerParams(collective_id=0, has_side_effects=True),
        )(tokens, w_gate, w_up, w_down)

    in_specs = (
        P(("dp", "row", "col"), None),
        P(("row", "col"), None),
        P(("row", "col"), None),
        P(None, ("row", "col")),
    )
    out_specs = P(("dp", "row", "col"), None)
    return jax.shard_map(shards, mesh=mesh, in_specs=in_specs, out_specs=out_specs, check_vma=False)
```

```python
import functools

import jax
import jax.numpy as jnp
from jax import lax
from jax.experimental import pallas as pl
from jax.experimental.pallas import tpu as pltpu
from jax.sharding import PartitionSpec as P

MESH = pl.DeviceIdType.MESH
CHUNKS = 4
SMALL_PART = 5, 16
LATER_PART = 16
EARLY_HOPS = 2
ORDER = (
    "fetch", "project 0", "project 1", "hop 1", "project 2", "project 3", "hop 2", "combine 0", "combine 1",
    "combine 2", "combine 3", "activate 0", "activate 1", "activate 2", "activate 3", "emit 0", "emit 1",
    "last hops", "local", "emit 2", "emit 3", "landed", "emit fetched",
)
X, A, B, C, D, HA, HB, OA, OB, FA, FB, ZA, ZB, MA, MB = range(15)


def tile_of(width, most):
    tile = min(width, most)
    while width % tile:
        tile //= 2
    return tile


def share_table(hidden, planes):
    even = hidden // planes
    later = even + even // LATER_PART // 16 * 16
    table = []
    for rows in (hidden - (planes - 1) * later, later):
        small = max(16, rows * SMALL_PART[0] // SMALL_PART[1] // 16 * 16)
        table.append((small, rows - small))
    return table


def kernel(
    groups, rows, cols, chunks,
    x_ref, wg_ref, wu_ref, wd_ref, out_ref,
    xin, wf, wg, wu, wa, wb, xbuf, acc, part, rec_a, rec_b, sum_a, sum_b, fin_a, fin_b, ha, hb, oa, ob,
    load_sem, sent_sem, x_sem, step_sem, fetch_sem, land_sem, mate_sem, out_sem,
):
    n = rows * cols
    row, col = lax.axis_index("row"), lax.axis_index("col")
    group = lax.axis_index("dp")
    mates = 2
    planes = groups // mates
    plane, core = group // mates, lax.rem(group, mates)
    count = x_ref.shape[0]
    t = count // chunks
    features, hidden = wg.shape
    half = hidden // 2
    side_cols = wa.shape[2]
    sizes = share_table(hidden, planes)
    bf16, f32 = jnp.bfloat16, jnp.float32

    def up(r, c):
        return lax.rem(row + r, rows), lax.rem(col + c, cols)

    def down(r, c):
        return lax.rem(row + rows - r, rows), lax.rem(col + cols - c, cols)

    def shard(rc, width):
        return pl.ds(pl.multiple_of((rc[0] * cols + rc[1]) * width, width), width)

    def remote(src, dst, kind, landing, to):
        return pltpu.make_async_remote_copy(
            src_ref=src, dst_ref=dst, send_sem=sent_sem.at[kind], recv_sem=landing,
            device_id={"row": to[0], "col": to[1]}, device_id_type=MESH,
        )

    def all_sent(kind, ref):
        remote(ref, ref, kind, out_sem.at[0], up(rows - 1, cols - 1)).wait_send()

    def all_here(landing, ref):
        remote(ref, ref, 0, landing, up(rows - 1, cols - 1)).wait_recv()

    def tok(k):
        return pl.ds(k * t, t)

    others = [(r, c) for r in range(rows) for c in range(cols)][1:]
    by_reach = others[::-1]
    rest_rows, rest_cols = pl.ds(1, rows - 1), pl.ds(1, cols - 1)

    def x_copy(k, r, c):
        to = up(r, c)
        return remote(
            xin.at[tok(k), shard(to, features)], xbuf.at[k, pl.ds((r * cols + c) * t, t)], X, x_sem.at[k], to
        )

    def a_copy(k, r):
        return remote(part.at[k, 0, r], rec_a.at[k, r], A, step_sem.at[0, k], down(r, 0))

    def b_copy(k, c):
        return remote(part.at[k, 1, :, c], rec_b.at[k, c], B, step_sem.at[1, k], down(0, c))

    def c_copy(k, c):
        return remote(sum_a.at[k, c], fin_a.at[k, c], C, step_sem.at[2, k], down(0, c))

    def d_copy(k, r):
        return remote(sum_b.at[k, r], fin_b.at[k, r], D, step_sem.at[3, k], down(r, 0))

    def ha_copy(k, r):
        return remote(ha.at[0, tok(k)], ha.at[r, tok(k)], HA, step_sem.at[4, k], up(r, 0))

    def hb_copy(k, c):
        return remote(hb.at[0, tok(k)], hb.at[c, tok(k)], HB, step_sem.at[5, k], up(0, c))

    def share_of(source, late, m):
        start = sum(sizes[0]) + (source - 1) * sum(sizes[1]) if late else 0
        if m:
            start = start + sizes[late][0]
        return pl.ds(pl.multiple_of(start, 16) if late else start, sizes[late][m])

    def as_core(do):
        for m in range(mates):

            @pl.when(core == m)
            def _():
                do(m)

    def as_self(do):
        for late in range(2):
            for m in range(mates):

                @pl.when(jnp.logical_and(core == m, plane > 0 if late else plane == 0))
                def _():
                    do(late, m)

    def fetch_a(late, m, c):
        return remote(
            wf.at[0, pl.ds(0, sizes[late][m])], wa.at[c, share_of(plane, late, m)], FA, fetch_sem.at[0], down(0, c)
        )

    def fetch_b(late, m, r):
        return remote(
            wf.at[1, pl.ds(0, sizes[late][m])], wb.at[r, share_of(plane, late, m)], FB, fetch_sem.at[1], down(r, 0)
        )

    sides = ((wa, rest_cols), (wb, rest_rows))

    def pass_on(source, side, late, m, to_plane):
        ref, rest = sides[side]
        region = ref.at[rest, share_of(source, late, m)]
        return pltpu.make_async_remote_copy(
            src_ref=region, dst_ref=region, send_sem=sent_sem.at[ZA + side], recv_sem=land_sem.at[source, side],
            device_id={"dp": to_plane * mates + core}, device_id_type=MESH,
        )

    def to_mate(source, side, late, m):
        ref, rest = sides[side]
        region = ref.at[rest, share_of(source, late, m)]
        return pltpu.make_async_remote_copy(
            src_ref=region, dst_ref=region, send_sem=sent_sem.at[MA + side], recv_sem=mate_sem.at[side],
            device_id={"dp": plane * mates + (mates - 1 - core)}, device_id_type=MESH,
        )

    def spread(source, side, late, m, upward, downward):
        if upward:
            pl.when(plane + 1 < planes)(lambda: pass_on(source, side, late, m, plane + 1).start())
        if downward:
            pl.when(plane > 0)(lambda: pass_on(source, side, late, m, plane - 1).start())
        to_mate(source, side, late, m).start()

    def hop(h):
        below, above = plane - h, plane + h

        def relay(m):
            for side in range(2):
                for late in range(2):

                    @pl.when(below > 0 if late else below == 0)
                    def _():
                        pass_on(below, side, late, m, plane).wait_recv()
                        spread(below, side, late, m, True, False)

                @pl.when(above < planes)
                def _():
                    pass_on(above, side, 1, m, plane).wait_recv()
                    spread(above, side, 1, m, False, True)

        as_core(relay)

    def rows_of(m):
        return sizes[0][m] + (planes - 1) * sizes[1][m]

    def last_hops():
        def more(h, _):
            hop(h)
            return 0

        lax.fori_loop(EARLY_HOPS + 1, planes, more, 0)

    def landed():
        def from_mate(m):
            for side, (ref, rest) in enumerate(sides):
                all_here(mate_sem.at[side], ref.at[rest, pl.ds(0, rows_of(1 - m))])

        as_core(from_mate)

    def columns(rc, side, start, width):
        base = (rc[0] * cols + rc[1]) * 2 * side_cols + side * side_cols + start
        return pl.ds(pl.multiple_of(base, width), width)

    def oa_copy(k, r):
        return remote(
            oa.at[0, r - 1, tok(k)], out_ref.at[tok(k), columns((row, col), 0, 0, side_cols)],
            OA, out_sem.at[0], down(r, 0),
        )

    def ob_copy(k, c):
        return remote(
            ob.at[0, c - 1, tok(k)], out_ref.at[tok(k), columns((row, col), 1, 0, side_cols)],
            OB, out_sem.at[1], down(0, c),
        )

    out_tile = tile_of(side_cols, 256)
    out_tiles = side_cols // out_tile

    def ga_copy(c, j, r):
        return remote(
            oa.at[c, r - 1, :, pl.ds(pl.multiple_of(j * out_tile, out_tile), out_tile)],
            out_ref.at[:, columns(up(0, c), 0, j * out_tile, out_tile)],
            OA, out_sem.at[0], down(r, 0),
        )

    def gb_copy(r, j, c):
        return remote(
            ob.at[r, c - 1, :, pl.ds(pl.multiple_of(j * out_tile, out_tile), out_tile)],
            out_ref.at[:, columns(up(r, 0), 1, j * out_tile, out_tile)],
            OB, out_sem.at[1], down(0, c),
        )

    def load_share(late, m):
        return [
            pltpu.make_async_copy(
                wd_ref.at[share_of(plane, late, m), pl.ds(side * side_cols, side_cols)],
                wf.at[side, pl.ds(0, sizes[late][m])], load_sem.at[side],
            )
            for side in range(2)
        ]

    load_tokens = pltpu.make_async_copy(x_ref, xin, load_sem.at[2])
    own = [
        pltpu.make_async_copy(
            x_ref.at[tok(k), shard((row, col), features)], xbuf.at[k, pl.ds(0, t)], load_sem.at[3 + k]
        )
        for k in range(chunks)
    ]
    loads = [
        pltpu.make_async_copy(wg_ref, wg, load_sem.at[3 + chunks]),
        pltpu.make_async_copy(wu_ref, wu, load_sem.at[4 + chunks]),
        pltpu.make_async_copy(wd_ref.at[:, pl.ds(0, side_cols)], wa.at[0], load_sem.at[5 + chunks]),
        pltpu.make_async_copy(wd_ref.at[:, pl.ds(side_cols, side_cols)], wb.at[0], load_sem.at[6 + chunks]),
    ]

    as_self(lambda late, m: [load.start() for load in load_share(late, m)])
    load_tokens.start()

    barrier = pltpu.get_barrier_semaphore()
    for r, c in others:
        to = up(r, c)
        pl.semaphore_signal(barrier, inc=1, device_id={"row": to[0], "col": to[1]}, device_id_type=MESH)

    def greet(g):
        pl.semaphore_signal(barrier, inc=1, device_id={"dp": g}, device_id_type=MESH)

    pl.when(plane > 0)(lambda: greet(group - mates))
    pl.when(plane + 1 < planes)(lambda: greet(group + mates))
    greet(plane * mates + (mates - 1 - core))
    neighbours = (plane > 0).astype(jnp.int32) + (plane + 1 < planes).astype(jnp.int32)
    as_self(lambda late, m: [load.wait() for load in load_share(late, m)])
    pl.semaphore_wait(barrier, n - 1 + mates - 1 + neighbours)

    def send_share(late, m):
        for c in range(1, cols):
            fetch_a(late, m, c).start()
        for r in range(1, rows):
            fetch_b(late, m, r).start()

    as_self(send_share)
    load_tokens.wait()
    for k in range(chunks):
        for r, c in by_reach:
            x_copy(k, r, c).start()
    for load in own + loads:
        load.start()

    def fetch():
        def take(late, m):
            for side, (ref, rest) in enumerate(sides):
                all_here(fetch_sem.at[side], ref.at[rest, share_of(plane, late, m)])
                spread(plane, side, late, m, True, True)

        as_self(take)
        for load in loads:
            load.wait()

    tile = tile_of(half, 512)
    per_half = half // tile

    def project(k):
        own[k].wait()
        all_here(x_sem.at[k], xbuf.at[k, pl.ds(t, (n - 1) * t)])

        def column(j, _):
            side, at = j // per_half, lax.rem(j, per_half) * tile
            source = pl.ds(pl.multiple_of(j * tile, tile), tile)
            for w, base in ((wg, 0), (wu, half)):
                target = pl.ds(pl.multiple_of(base + at, tile), tile)
                got = jnp.dot(xbuf[k], w[:, source], preferred_element_type=f32)
                acc[k, side, :, target] = got[:t]
                for r, c in others:
                    first = (r * cols + c) * t
                    part[k, side, r, c, :, target] = got[first : first + t].astype(bf16)
            return 0

        lax.fori_loop(0, 2 * per_half, column, 0)
        for r in range(1, rows):
            a_copy(k, r).start()
        for c in range(1, cols):
            b_copy(k, c).start()

    def combine(k):
        all_here(step_sem.at[0, k], rec_a.at[k, rest_rows])
        for c in range(1, cols):
            total = part[k, 0, 0, c].astype(f32)
            for r in range(1, rows):
                total = total + rec_a[k, r, c].astype(f32)
            sum_a[k, c] = total.astype(bf16)
            c_copy(k, c).start()
        all_here(step_sem.at[1, k], rec_b.at[k, rest_cols])
        for r in range(1, rows):
            total = part[k, 1, r, 0].astype(f32)
            for c in range(1, cols):
                total = total + rec_b[k, c, r].astype(f32)
            sum_b[k, r] = total.astype(bf16)
            d_copy(k, r).start()

    def activate(k):
        all_here(step_sem.at[2, k], fin_a.at[k, rest_cols])
        all_here(step_sem.at[3, k], fin_b.at[k, rest_rows])
        for side in range(2):
            total = acc[k, side]
            if side == 0:
                for r in range(1, rows):
                    total = total + rec_a[k, r, 0].astype(f32)
                for c in range(1, cols):
                    total = total + fin_a[k, c].astype(f32)
            else:
                for c in range(1, cols):
                    total = total + rec_b[k, c, 0].astype(f32)
                for r in range(1, rows):
                    total = total + fin_b[k, r].astype(f32)
            gate = total[:, :half]
            done = (gate / (1.0 + jnp.exp(-gate)) * total[:, half:]).astype(bf16)
            ha[0, tok(k), pl.ds(side * half, half)] = done
            hb[0, tok(k), pl.ds(side * half, half)] = done
        for r in range(1, rows):
            ha_copy(k, r).start()
        for c in range(1, cols):
            hb_copy(k, c).start()

    wide = tile_of(side_cols, 512)
    wides = side_cols // wide

    def emit(k):
        all_here(step_sem.at[4, k], ha.at[rest_rows, tok(k)])
        theirs = ha[rest_rows, tok(k)].reshape((rows - 1) * t, hidden)
        for j in range(wides):
            where = pl.ds(j * wide, wide)
            got = jnp.dot(theirs, wa[0, :, where], preferred_element_type=f32).astype(bf16)
            oa[0, :, tok(k), where] = got.reshape(rows - 1, t, wide)
        for r in range(1, rows):
            oa_copy(k, r).start()
        all_here(step_sem.at[5, k], hb.at[rest_cols, tok(k)])
        theirs = hb[rest_cols, tok(k)].reshape((cols - 1) * t, hidden)
        for j in range(wides):
            where = pl.ds(j * wide, wide)
            got = jnp.dot(theirs, wb[0, :, where], preferred_element_type=f32).astype(bf16)
            ob[0, :, tok(k), where] = got.reshape(cols - 1, t, wide)
        for c in range(1, cols):
            ob_copy(k, c).start()

    def local():
        def columns_of(j, _):
            where = pl.ds(pl.multiple_of(j * wide, wide), wide)
            for side, w in ((0, wa), (1, wb)):
                out_ref[:, columns((row, col), side, j * wide, wide)] = jnp.dot(
                    ha[0], w[0, :, where], preferred_element_type=f32
                ).astype(bf16)
            return 0

        lax.fori_loop(0, wides, columns_of, 0)

    def fetched_a(i):
        c, j = 1 + i // out_tiles, lax.rem(i, out_tiles)
        where = pl.ds(pl.multiple_of(j * out_tile, out_tile), out_tile)
        got = jnp.dot(
            ha[...].reshape(rows * count, hidden), wa[c, :, where], preferred_element_type=f32
        ).astype(bf16)
        oa[c, :, :, where] = got[count:].reshape(rows - 1, count, out_tile)
        out_ref[:, columns(up(0, c), 0, j * out_tile, out_tile)] = got[:count]
        for r in range(1, rows):
            ga_copy(c, j, r).start()

    def fetched_b(i):
        r, j = 1 + i // out_tiles, lax.rem(i, out_tiles)
        where = pl.ds(pl.multiple_of(j * out_tile, out_tile), out_tile)
        got = jnp.dot(
            hb[...].reshape(cols * count, hidden), wb[r, :, where], preferred_element_type=f32
        ).astype(bf16)
        ob[r, :, :, where] = got[count:].reshape(cols - 1, count, out_tile)
        out_ref[:, columns(up(r, 0), 1, j * out_tile, out_tile)] = got[:count]
        for c in range(1, cols):
            gb_copy(r, j, c).start()

    tiles_a, tiles_b = (cols - 1) * out_tiles, (rows - 1) * out_tiles
    both = min(tiles_a, tiles_b)

    def emit_fetched():
        def pair(i, _):
            fetched_a(i)
            fetched_b(i)
            return 0

        def only(one):
            def body(i, _):
                one(i)
                return 0

            return body

        lax.fori_loop(0, both, pair, 0)
        lax.fori_loop(both, tiles_a, only(fetched_a), 0)
        lax.fori_loop(both, tiles_b, only(fetched_b), 0)

    stages = {"project": project, "combine": combine, "activate": activate, "emit": emit}
    once = {
        "fetch": fetch, "last hops": last_hops, "landed": landed, "local": local, "emit fetched": emit_fetched,
    }
    for task in ORDER:
        if task in once:
            once[task]()
        else:
            name, at = task.split()
            if name == "hop":
                if int(at) < planes:
                    hop(int(at))
            else:
                stages[name](int(at))

    all_sent(X, xbuf.at[:, pl.ds(t, (n - 1) * t)])
    all_sent(A, rec_a.at[:, rest_rows])
    all_sent(B, rec_b.at[:, rest_cols])
    all_sent(C, fin_a.at[:, rest_cols])
    all_sent(D, fin_b.at[:, rest_rows])
    all_sent(HA, ha.at[rest_rows])
    all_sent(HB, hb.at[rest_cols])

    def shares_sent(late, m):
        for side, (ref, rest) in enumerate(sides):

            def drained(kind, size):
                all_sent(kind + side, ref.at[rest, pl.ds(0, size)])

            drained(FA, sizes[late][m])
            drained(MA, rows_of(m))
            if not late:
                if planes > 1:
                    drained(ZA, sizes[0][m])
                continue
            inner = plane + 1 < planes
            pl.when(inner)(lambda: drained(ZA, rows_of(m) + sizes[1][m]))
            pl.when(jnp.logical_not(inner))(lambda: drained(ZA, sizes[1][m]))

    as_self(shares_sent)
    all_sent(OA, oa)
    all_sent(OB, ob)
    all_here(out_sem.at[0], oa)
    all_here(out_sem.at[1], ob)


def solution(mesh):
    groups, rows, cols = mesh.shape["dp"], mesh.shape["row"], mesh.shape["col"]
    planes = groups // 2
    n = rows * cols

    def shards(tokens, w_gate, w_up, w_down):
        count, width = tokens.shape
        features, hidden = w_gate.shape
        side_cols = w_down.shape[1] // 2
        largest = max(map(max, share_table(hidden, planes)))
        chunks = CHUNKS
        t = count // chunks
        bf16 = jnp.bfloat16
        any_space = pl.BlockSpec(memory_space=pl.ANY)
        dma = pltpu.SemaphoreType.DMA

        return pl.pallas_call(
            functools.partial(kernel, groups, rows, cols, chunks),
            out_shape=pltpu.VMEM((count, width), bf16),
            in_specs=[any_space] * 4,
            out_specs=pl.BlockSpec(memory_space=pltpu.VMEM),
            scratch_shapes=[
                pltpu.VMEM((count, width), bf16),
                pltpu.VMEM((2, largest, side_cols), bf16),
                pltpu.VMEM((features, hidden), bf16),
                pltpu.VMEM((features, hidden), bf16),
                pltpu.VMEM((cols, hidden, side_cols), bf16),
                pltpu.VMEM((rows, hidden, side_cols), bf16),
                pltpu.VMEM((chunks, n * t, features), bf16),
                pltpu.VMEM((chunks, 2, t, hidden), jnp.float32),
                pltpu.VMEM((chunks, 2, rows, cols, t, hidden), bf16),
                pltpu.VMEM((chunks, rows, cols, t, hidden), bf16),
                pltpu.VMEM((chunks, cols, rows, t, hidden), bf16),
                pltpu.VMEM((chunks, cols, t, hidden), bf16),
                pltpu.VMEM((chunks, rows, t, hidden), bf16),
                pltpu.VMEM((chunks, cols, t, hidden), bf16),
                pltpu.VMEM((chunks, rows, t, hidden), bf16),
                pltpu.VMEM((rows, count, hidden), bf16),
                pltpu.VMEM((cols, count, hidden), bf16),
                pltpu.VMEM((cols, rows - 1, count, side_cols), bf16),
                pltpu.VMEM((rows, cols - 1, count, side_cols), bf16),
                dma((7 + chunks,)),
                dma((15,)),
                dma((chunks,)),
                dma((6, chunks)),
                dma((2,)),
                dma((planes, 2)),
                dma((2,)),
                dma((2,)),
            ],
            compiler_params=pltpu.CompilerParams(collective_id=0, has_side_effects=True),
        )(tokens, w_gate, w_up, w_down)

    in_specs = (
        P(("dp", "row", "col"), None),
        P(("row", "col"), None),
        P(("row", "col"), None),
        P(None, ("row", "col")),
    )
    out_specs = P(("dp", "row", "col"), None)
    return jax.shard_map(shards, mesh=mesh, in_specs=in_specs, out_specs=out_specs, check_vma=False)
```

```python
import functools

import jax
import jax.numpy as jnp
from jax import lax
from jax.experimental import pallas as pl
from jax.experimental.pallas import tpu as pltpu
from jax.sharding import PartitionSpec as P

MESH = pl.DeviceIdType.MESH
CHUNKS = 4
SMALL_PART = 5, 16
LATER_PART = 16
EARLY_HOPS = 2
ORDER = (
    "fetch", "project 0", "project 1", "hop 1", "project 2", "project 3", "hop 2", "combine 0", "combine 1",
    "combine 2", "combine 3", "activate 0", "activate 1", "activate 2", "activate 3", "emit 0", "emit 1",
    "last hops", "local", "emit 2", "emit 3", "landed", "emit fetched",
)
X, AB, CD, H, OA, OB, FA, FB, ZA, ZB, MA, MB = range(12)


def tile_of(width, most):
    tile = min(width, most)
    while width % tile:
        tile //= 2
    return tile


def share_table(hidden, planes):
    even = hidden // planes
    later = even + even // LATER_PART // 16 * 16
    table = []
    for rows in (hidden - (planes - 1) * later, later):
        small = max(16, rows * SMALL_PART[0] // SMALL_PART[1] // 16 * 16)
        table.append((small, rows - small))
    return table


def kernel(
    groups, rows, cols, chunks,
    x_ref, wg_ref, wu_ref, wd_ref, out_ref,
    xin, wf, wg, wu, wa, wb, xbuf, acc, part, rec, sum_a, sum_b, fin, held, oa, ob,
    load_sem, sent_sem, x_sem, step_sem, fetch_sem, land_sem, mate_sem, out_sem,
):
    n = rows * cols
    row, col = lax.axis_index("row"), lax.axis_index("col")
    group = lax.axis_index("dp")
    mates = 2
    planes = groups // mates
    plane, core = group // mates, lax.rem(group, mates)
    count = x_ref.shape[0]
    t = count // chunks
    features, hidden = wg.shape
    half = hidden // 2
    side_cols = wa.shape[2]
    sizes = share_table(hidden, planes)
    bf16, f32 = jnp.bfloat16, jnp.float32

    def up(r, c):
        return lax.rem(row + r, rows), lax.rem(col + c, cols)

    def down(r, c):
        return lax.rem(row + rows - r, rows), lax.rem(col + cols - c, cols)

    def shard(rc, width):
        return pl.ds(pl.multiple_of((rc[0] * cols + rc[1]) * width, width), width)

    def remote(src, dst, kind, landing, to):
        return pltpu.make_async_remote_copy(
            src_ref=src, dst_ref=dst, send_sem=sent_sem.at[kind], recv_sem=landing,
            device_id={"row": to[0], "col": to[1]}, device_id_type=MESH,
        )

    def all_sent(kind, ref):
        remote(ref, ref, kind, out_sem.at[0], up(rows - 1, cols - 1)).wait_send()

    def all_here(landing, ref):
        remote(ref, ref, 0, landing, up(rows - 1, cols - 1)).wait_recv()

    def tok(k):
        return pl.ds(k * t, t)

    others = [(r, c) for r in range(rows) for c in range(cols)][1:]
    by_reach = others[::-1]
    rest_rows, rest_cols = pl.ds(1, rows - 1), pl.ds(1, cols - 1)

    def x_copy(k, r, c):
        to = up(r, c)
        return remote(
            xin.at[tok(k), shard(to, features)], xbuf.at[k, pl.ds((r * cols + c) * t, t)], X, x_sem.at[k], to
        )

    from_b = (rows - 1) * cols

    def at_a(r, c):
        return (r - 1) * cols + c

    def at_b(c, r):
        return from_b + (c - 1) * rows + r

    def a_copy(k, r):
        return remote(part.at[k, 0, r], rec.at[k, pl.ds(at_a(r, 0), cols)], AB, step_sem.at[0, k], down(r, 0))

    def b_copy(k, c):
        return remote(part.at[k, 1, :, c], rec.at[k, pl.ds(at_b(c, 0), rows)], AB, step_sem.at[0, k], down(0, c))

    def c_copy(k, c):
        return remote(sum_a.at[k, c], fin.at[k, c - 1], CD, step_sem.at[1, k], down(0, c))

    def d_copy(k, r):
        return remote(sum_b.at[k, r], fin.at[k, cols - 2 + r], CD, step_sem.at[1, k], down(r, 0))

    mine = rows - 1
    from_rows, from_cols = pl.ds(0, rows - 1), pl.ds(rows, cols - 1)

    def ha_copy(k, r):
        return remote(held.at[mine, tok(k)], held.at[r - 1, tok(k)], H, step_sem.at[2, k], up(r, 0))

    def hb_copy(k, c):
        return remote(held.at[mine, tok(k)], held.at[mine + c, tok(k)], H, step_sem.at[2, k], up(0, c))

    def share_of(source, late, m):
        start = sum(sizes[0]) + (source - 1) * sum(sizes[1]) if late else 0
        if m:
            start = start + sizes[late][0]
        return pl.ds(pl.multiple_of(start, 16) if late else start, sizes[late][m])

    def as_core(do):
        for m in range(mates):

            @pl.when(core == m)
            def _():
                do(m)

    def as_self(do):
        for late in range(2):
            for m in range(mates):

                @pl.when(jnp.logical_and(core == m, plane > 0 if late else plane == 0))
                def _():
                    do(late, m)

    def fetch_a(late, m, c):
        return remote(
            wf.at[0, pl.ds(0, sizes[late][m])], wa.at[c, share_of(plane, late, m)], FA, fetch_sem.at[0], down(0, c)
        )

    def fetch_b(late, m, r):
        return remote(
            wf.at[1, pl.ds(0, sizes[late][m])], wb.at[r, share_of(plane, late, m)], FB, fetch_sem.at[1], down(r, 0)
        )

    sides = ((wa, rest_cols), (wb, rest_rows))

    def pass_on(source, side, late, m, to_plane):
        ref, rest = sides[side]
        region = ref.at[rest, share_of(source, late, m)]
        return pltpu.make_async_remote_copy(
            src_ref=region, dst_ref=region, send_sem=sent_sem.at[ZA + side], recv_sem=land_sem.at[source, side],
            device_id={"dp": to_plane * mates + core}, device_id_type=MESH,
        )

    def to_mate(source, side, late, m):
        ref, rest = sides[side]
        region = ref.at[rest, share_of(source, late, m)]
        return pltpu.make_async_remote_copy(
            src_ref=region, dst_ref=region, send_sem=sent_sem.at[MA + side], recv_sem=mate_sem.at[side],
            device_id={"dp": plane * mates + (mates - 1 - core)}, device_id_type=MESH,
        )

    def spread(source, side, late, m, upward, downward):
        if upward:
            pl.when(plane + 1 < planes)(lambda: pass_on(source, side, late, m, plane + 1).start())
        if downward:
            pl.when(plane > 0)(lambda: pass_on(source, side, late, m, plane - 1).start())
        to_mate(source, side, late, m).start()

    def hop(h):
        below, above = plane - h, plane + h

        def relay(m):
            for side in range(2):
                for late in range(2):

                    @pl.when(below > 0 if late else below == 0)
                    def _():
                        pass_on(below, side, late, m, plane).wait_recv()
                        spread(below, side, late, m, True, False)

                @pl.when(above < planes)
                def _():
                    pass_on(above, side, 1, m, plane).wait_recv()
                    spread(above, side, 1, m, False, True)

        as_core(relay)

    def rows_of(m):
        return sizes[0][m] + (planes - 1) * sizes[1][m]

    def last_hops():
        def more(h, _):
            hop(h)
            return 0

        lax.fori_loop(EARLY_HOPS + 1, planes, more, 0)

    def landed():
        def from_mate(m):
            for side, (ref, rest) in enumerate(sides):
                all_here(mate_sem.at[side], ref.at[rest, pl.ds(0, rows_of(1 - m))])

        as_core(from_mate)

    def columns(rc, side, start, width):
        base = (rc[0] * cols + rc[1]) * 2 * side_cols + side * side_cols + start
        return pl.ds(pl.multiple_of(base, width), width)

    def oa_copy(k, r):
        return remote(
            oa.at[0, r - 1, tok(k)], out_ref.at[tok(k), columns((row, col), 0, 0, side_cols)],
            OA, out_sem.at[0], down(r, 0),
        )

    def ob_copy(k, c):
        return remote(
            ob.at[0, c - 1, tok(k)], out_ref.at[tok(k), columns((row, col), 1, 0, side_cols)],
            OB, out_sem.at[1], down(0, c),
        )

    out_tile = tile_of(side_cols, 256)
    out_tiles = side_cols // out_tile

    def ga_copy(c, j, r):
        return remote(
            oa.at[c, r - 1, :, pl.ds(pl.multiple_of(j * out_tile, out_tile), out_tile)],
            out_ref.at[:, columns(up(0, c), 0, j * out_tile, out_tile)],
            OA, out_sem.at[0], down(r, 0),
        )

    def gb_copy(r, j, c):
        return remote(
            ob.at[r, c - 1, :, pl.ds(pl.multiple_of(j * out_tile, out_tile), out_tile)],
            out_ref.at[:, columns(up(r, 0), 1, j * out_tile, out_tile)],
            OB, out_sem.at[1], down(0, c),
        )

    def load_share(late, m):
        return [
            pltpu.make_async_copy(
                wd_ref.at[share_of(plane, late, m), pl.ds(side * side_cols, side_cols)],
                wf.at[side, pl.ds(0, sizes[late][m])], load_sem.at[side],
            )
            for side in range(2)
        ]

    load_tokens = pltpu.make_async_copy(x_ref, xin, load_sem.at[2])
    own = [
        pltpu.make_async_copy(
            x_ref.at[tok(k), shard((row, col), features)], xbuf.at[k, pl.ds(0, t)], load_sem.at[3 + k]
        )
        for k in range(chunks)
    ]
    loads = [
        pltpu.make_async_copy(wg_ref, wg, load_sem.at[3 + chunks]),
        pltpu.make_async_copy(wu_ref, wu, load_sem.at[4 + chunks]),
        pltpu.make_async_copy(wd_ref.at[:, pl.ds(0, side_cols)], wa.at[0], load_sem.at[5 + chunks]),
        pltpu.make_async_copy(wd_ref.at[:, pl.ds(side_cols, side_cols)], wb.at[0], load_sem.at[6 + chunks]),
    ]

    as_self(lambda late, m: [load.start() for load in load_share(late, m)])
    load_tokens.start()

    barrier = pltpu.get_barrier_semaphore()
    for r, c in others:
        to = up(r, c)
        pl.semaphore_signal(barrier, inc=1, device_id={"row": to[0], "col": to[1]}, device_id_type=MESH)

    def greet(g):
        pl.semaphore_signal(barrier, inc=1, device_id={"dp": g}, device_id_type=MESH)

    pl.when(plane > 0)(lambda: greet(group - mates))
    pl.when(plane + 1 < planes)(lambda: greet(group + mates))
    greet(plane * mates + (mates - 1 - core))
    neighbours = (plane > 0).astype(jnp.int32) + (plane + 1 < planes).astype(jnp.int32)
    pl.semaphore_wait(barrier, n - 1 + mates - 1 + neighbours)

    def send_share(late, m):
        share_a, share_b = load_share(late, m)
        share_a.wait()
        for c in range(1, cols):
            fetch_a(late, m, c).start()
        share_b.wait()
        for r in range(1, rows):
            fetch_b(late, m, r).start()

    as_self(send_share)
    load_tokens.wait()
    for k in range(chunks):
        for r, c in by_reach:
            x_copy(k, r, c).start()
    for load in own + loads:
        load.start()

    def fetch():
        def take(late, m):
            for side, (ref, rest) in enumerate(sides):
                all_here(fetch_sem.at[side], ref.at[rest, share_of(plane, late, m)])
                spread(plane, side, late, m, True, True)

        as_self(take)
        for load in loads:
            load.wait()

    tile = tile_of(half, 512)
    per_half = half // tile

    def project(k):
        own[k].wait()
        all_here(x_sem.at[k], xbuf.at[k, pl.ds(t, (n - 1) * t)])

        def column(j, _):
            side, at = j // per_half, lax.rem(j, per_half) * tile
            source = pl.ds(pl.multiple_of(j * tile, tile), tile)
            for w, base in ((wg, 0), (wu, half)):
                target = pl.ds(pl.multiple_of(base + at, tile), tile)
                got = jnp.dot(xbuf[k], w[:, source], preferred_element_type=f32)
                acc[k, side, :, target] = got[:t]
                for r, c in others:
                    first = (r * cols + c) * t
                    part[k, side, r, c, :, target] = got[first : first + t].astype(bf16)
            return 0

        lax.fori_loop(0, 2 * per_half, column, 0)
        for r in range(1, rows):
            a_copy(k, r).start()
        for c in range(1, cols):
            b_copy(k, c).start()

    def combine(k):
        all_here(step_sem.at[0, k], rec.at[k])
        for c in range(1, cols):
            total = part[k, 0, 0, c].astype(f32)
            for r in range(1, rows):
                total = total + rec[k, at_a(r, c)].astype(f32)
            sum_a[k, c] = total.astype(bf16)
            c_copy(k, c).start()
        for r in range(1, rows):
            total = part[k, 1, r, 0].astype(f32)
            for c in range(1, cols):
                total = total + rec[k, at_b(c, r)].astype(f32)
            sum_b[k, r] = total.astype(bf16)
            d_copy(k, r).start()

    def activate(k):
        all_here(step_sem.at[1, k], fin.at[k])
        for side in range(2):
            total = acc[k, side]
            if side == 0:
                for r in range(1, rows):
                    total = total + rec[k, at_a(r, 0)].astype(f32)
                for c in range(1, cols):
                    total = total + fin[k, c - 1].astype(f32)
            else:
                for c in range(1, cols):
                    total = total + rec[k, at_b(c, 0)].astype(f32)
                for r in range(1, rows):
                    total = total + fin[k, cols - 2 + r].astype(f32)
            gate = total[:, :half]
            done = (gate / (1.0 + jnp.exp(-gate)) * total[:, half:]).astype(bf16)
            held[mine, tok(k), pl.ds(side * half, half)] = done
        for r in range(1, rows):
            ha_copy(k, r).start()
        for c in range(1, cols):
            hb_copy(k, c).start()

    wide = tile_of(side_cols, 512)
    wides = side_cols // wide

    def emit(k):
        all_here(step_sem.at[2, k], held.at[pl.ds(0, rows + cols - 2), tok(k)])
        theirs = held[from_rows, tok(k)].reshape((rows - 1) * t, hidden)
        for j in range(wides):
            where = pl.ds(j * wide, wide)
            got = jnp.dot(theirs, wa[0, :, where], preferred_element_type=f32).astype(bf16)
            oa[0, :, tok(k), where] = got.reshape(rows - 1, t, wide)
        for r in range(1, rows):
            oa_copy(k, r).start()
        theirs = held[from_cols, tok(k)].reshape((cols - 1) * t, hidden)
        for j in range(wides):
            where = pl.ds(j * wide, wide)
            got = jnp.dot(theirs, wb[0, :, where], preferred_element_type=f32).astype(bf16)
            ob[0, :, tok(k), where] = got.reshape(cols - 1, t, wide)
        for c in range(1, cols):
            ob_copy(k, c).start()

    def local():
        def columns_of(j, _):
            where = pl.ds(pl.multiple_of(j * wide, wide), wide)
            for side, w in ((0, wa), (1, wb)):
                out_ref[:, columns((row, col), side, j * wide, wide)] = jnp.dot(
                    held[mine], w[0, :, where], preferred_element_type=f32
                ).astype(bf16)
            return 0

        lax.fori_loop(0, wides, columns_of, 0)

    def fetched_a(i):
        c, j = 1 + i // out_tiles, lax.rem(i, out_tiles)
        where = pl.ds(pl.multiple_of(j * out_tile, out_tile), out_tile)
        got = jnp.dot(
            held[pl.ds(0, rows)].reshape(rows * count, hidden), wa[c, :, where], preferred_element_type=f32
        ).astype(bf16)
        oa[c, :, :, where] = got[: mine * count].reshape(rows - 1, count, out_tile)
        out_ref[:, columns(up(0, c), 0, j * out_tile, out_tile)] = got[mine * count :]
        for r in range(1, rows):
            ga_copy(c, j, r).start()

    def fetched_b(i):
        r, j = 1 + i // out_tiles, lax.rem(i, out_tiles)
        where = pl.ds(pl.multiple_of(j * out_tile, out_tile), out_tile)
        got = jnp.dot(
            held[pl.ds(mine, cols)].reshape(cols * count, hidden), wb[r, :, where], preferred_element_type=f32
        ).astype(bf16)
        ob[r, :, :, where] = got[count:].reshape(cols - 1, count, out_tile)
        out_ref[:, columns(up(r, 0), 1, j * out_tile, out_tile)] = got[:count]
        for c in range(1, cols):
            gb_copy(r, j, c).start()

    tiles_a, tiles_b = (cols - 1) * out_tiles, (rows - 1) * out_tiles
    both = min(tiles_a, tiles_b)

    def emit_fetched():
        def pair(i, _):
            fetched_a(i)
            fetched_b(i)
            return 0

        def only(one):
            def body(i, _):
                one(i)
                return 0

            return body

        lax.fori_loop(0, both, pair, 0)
        lax.fori_loop(both, tiles_a, only(fetched_a), 0)
        lax.fori_loop(both, tiles_b, only(fetched_b), 0)

    stages = {"project": project, "combine": combine, "activate": activate, "emit": emit}
    once = {
        "fetch": fetch, "last hops": last_hops, "landed": landed, "local": local, "emit fetched": emit_fetched,
    }
    for task in ORDER:
        if task in once:
            once[task]()
        else:
            name, at = task.split()
            if name == "hop":
                if int(at) < planes:
                    hop(int(at))
            else:
                stages[name](int(at))

    all_sent(X, xbuf.at[:, pl.ds(t, (n - 1) * t)])
    all_sent(AB, rec)
    all_sent(CD, fin)
    all_sent(H, held.at[pl.ds(0, rows + cols - 2)])

    def shares_sent(late, m):
        for side, (ref, rest) in enumerate(sides):

            def drained(kind, size):
                all_sent(kind + side, ref.at[rest, pl.ds(0, size)])

            drained(FA, sizes[late][m])
            drained(MA, rows_of(m))
            if not late:
                if planes > 1:
                    drained(ZA, sizes[0][m])
                continue
            inner = plane + 1 < planes
            pl.when(inner)(lambda: drained(ZA, rows_of(m) + sizes[1][m]))
            pl.when(jnp.logical_not(inner))(lambda: drained(ZA, sizes[1][m]))

    as_self(shares_sent)
    all_sent(OA, oa)
    all_sent(OB, ob)
    all_here(out_sem.at[0], oa)
    all_here(out_sem.at[1], ob)


def solution(mesh):
    groups, rows, cols = mesh.shape["dp"], mesh.shape["row"], mesh.shape["col"]
    planes = groups // 2
    n = rows * cols

    def shards(tokens, w_gate, w_up, w_down):
        count, width = tokens.shape
        features, hidden = w_gate.shape
        side_cols = w_down.shape[1] // 2
        largest = max(map(max, share_table(hidden, planes)))
        chunks = CHUNKS
        t = count // chunks
        bf16 = jnp.bfloat16
        any_space = pl.BlockSpec(memory_space=pl.ANY)
        dma = pltpu.SemaphoreType.DMA

        return pl.pallas_call(
            functools.partial(kernel, groups, rows, cols, chunks),
            out_shape=pltpu.VMEM((count, width), bf16),
            in_specs=[any_space] * 4,
            out_specs=pl.BlockSpec(memory_space=pltpu.VMEM),
            scratch_shapes=[
                pltpu.VMEM((count, width), bf16),
                pltpu.VMEM((2, largest, side_cols), bf16),
                pltpu.VMEM((features, hidden), bf16),
                pltpu.VMEM((features, hidden), bf16),
                pltpu.VMEM((cols, hidden, side_cols), bf16),
                pltpu.VMEM((rows, hidden, side_cols), bf16),
                pltpu.VMEM((chunks, n * t, features), bf16),
                pltpu.VMEM((chunks, 2, t, hidden), jnp.float32),
                pltpu.VMEM((chunks, 2, rows, cols, t, hidden), bf16),
                pltpu.VMEM((chunks, (rows - 1) * cols + (cols - 1) * rows, t, hidden), bf16),
                pltpu.VMEM((chunks, cols, t, hidden), bf16),
                pltpu.VMEM((chunks, rows, t, hidden), bf16),
                pltpu.VMEM((chunks, rows + cols - 2, t, hidden), bf16),
                pltpu.VMEM((rows + cols - 1, count, hidden), bf16),
                pltpu.VMEM((cols, rows - 1, count, side_cols), bf16),
                pltpu.VMEM((rows, cols - 1, count, side_cols), bf16),
                dma((7 + chunks,)),
                dma((12,)),
                dma((chunks,)),
                dma((3, chunks)),
                dma((2,)),
                dma((planes, 2)),
                dma((2,)),
                dma((2,)),
            ],
            compiler_params=pltpu.CompilerParams(collective_id=0, has_side_effects=True),
        )(tokens, w_gate, w_up, w_down)

    in_specs = (
        P(("dp", "row", "col"), None),
        P(("row", "col"), None),
        P(("row", "col"), None),
        P(None, ("row", "col")),
    )
    out_specs = P(("dp", "row", "col"), None)
    return jax.shard_map(shards, mesh=mesh, in_specs=in_specs, out_specs=out_specs, check_vma=False)
```
